256 devices in a mesh: mem: 4 (over z_hi, core), lat: 64 (over z_lo, x, y).
Axes of the slice: x: 4, y: 4, z: 8 (z_hi: 2, z_lo: 4; z = z_hi * 4 + z_lo), core: 2. Of those that a mesh axis runs over, the one named last changes fastest.
Arguments:
- control: float32 [128, 128, 1024], P('mem', 'lat'), may hold values from -6 to 6
- ensemble: float32 [128, 4, 128, 1024], P('mem', None, 'lat'), may hold values from -0.72 to 0.72
- widths: int32 [128], P('lat'), may hold values from 0 to 4
- interp_source: int32 [4, 256, 2048], P(None, 'lat'), may hold values from 0 to 4095, as said below
- interp_weight: float32 [4, 256, 2048], P(None, 'lat'), may hold values from 0.1 to 0.5
- obs_mask: int32 [4, 256, 2048], P(None, 'lat'), may hold values 0 or 1
- innovation: float32 [4, 256, 2048], P(None, 'lat'), may hold values from -12 to 12
Outputs:
- control_next: float32 [128, 128, 1024], P('mem', 'lat')
The draws below stay inside these ranges and needn't reach their ends.
Inputs may be any that keep to these rules, and one draw needn't show every extreme that they name: `interp_source`: for a fine point (j, i) in band b = j // 4 each value is (row - b * 2 + 1) * 1024 + column of a coarse cell inside the grid whose row differs from j // 2 by at most 1 and whose column differs from i // 2 by at most 2, cyclically modulo 1024.
All inputs are finite; a program needn't handle non-finite values. No bound on the sum of `obs_mask` on one device may be relied on, other than what follows from the above.
Results may differ from the reference program's by a relative error of at most 0.0001.
Values sent between devices are 32-bit elements; how exact they have to be, the bound alone decides.
No kernel may reach another device: no remote copies, remote signals or barrier semaphores. Data moves between devices by JAX's collectives and lax.ppermute only.
A program may use at most 128 MiB of HBM per device.

```python
import jax
import jax.numpy as jnp
from jax import lax

CLAT = 2
NLON = 1024
NT = 4
WIDEST = 4
GRAD_STEPS = 2
MEMBERS = 128
NLAT = 128
FLON = 2048
NFLAT = 256


def draw_interp_source(key, part):
    key_rows, key_cols = jax.random.split(jax.random.fold_in(key, 7), 2)
    fine_rows = jnp.arange(NFLAT, dtype=jnp.int32)
    band_first = fine_rows // (2 * CLAT) * CLAT
    base_row = fine_rows // 2
    jitter = jax.random.randint(key_rows, (4, NFLAT, FLON), -1, 2)
    coarse_row = base_row[None, :, None] + jitter
    lowest = jnp.maximum(band_first - 1, 0)[None, :, None]
    highest = jnp.minimum(band_first + CLAT, NLAT - 1)[None, :, None]
    coarse_row = jnp.clip(coarse_row, lowest, highest)
    base_col = jnp.arange(FLON, dtype=jnp.int32) // 2
    coarse_col = (base_col[None, None, :] + jax.random.randint(key_cols, (4, NFLAT, FLON), -2, 3)) % NLON
    return ((coarse_row - band_first[None, :, None] + 1) * NLON + coarse_col).astype(jnp.int32)


def set_ends(values, stream_key, least, high):
    longest = values.shape.index(max(values.shape))
    spots = []
    for shift in (0, 1):
        where = [jax.random.randint(jax.random.fold_in(stream_key, axis), (), 0, length) for axis, length in enumerate(values.shape)]
        where[longest] = (where[longest] + shift) % values.shape[longest]
        spots.append(tuple(where))
    return values.at[spots[0]].set(least).at[spots[1]].set(high)


def block_scale(rng, extent, cuts, low, largest):
    loudness, own = 1.0, jax.random.fold_in(rng, 6)
    for dim, parts in cuts:
        heights = jnp.exp(jax.random.uniform(jax.random.fold_in(own, dim), (parts,), jnp.float32, low / len(cuts), largest / len(cuts)))
        loudness = loudness * jnp.repeat(heights, extent[dim] // parts).reshape([-1 if axis == dim else 1 for axis in range(len(extent))])
    return loudness


def scatter_about(stream_key, shape, deviation, limit, cuts=(), kind=jnp.bfloat16):
    loudness = block_scale(stream_key, shape, cuts, -0.22, 0.18) if cuts else 1.0
    result = jax.random.normal(stream_key, shape, jnp.float32) * deviation * loudness
    return jnp.minimum(jnp.maximum(result, -limit), limit).astype(kind)


def setup_inputs(seed: int = 0) -> dict:
    splits = jax.random.split(jax.random.key(seed), 8)
    return {
        "control": scatter_about(splits[0], (MEMBERS, NLAT, NLON), 1.0, 6.0, ((0, 4), (1, 64)), jnp.float32),
        "ensemble": scatter_about(splits[1], (MEMBERS, NT, NLAT, NLON), 0.12, 0.72, ((0, 4), (2, 64)), jnp.float32),
        "widths": set_ends(jax.random.randint(splits[2], (NLAT,), 0, WIDEST + 1), jax.random.fold_in(splits[2], 1), 0, WIDEST).astype(jnp.int32),
        "interp_source": draw_interp_source(jax.random.fold_in(splits[7], 71), 0),
        "interp_weight": jnp.clip(0.1 + 0.4 * jax.random.uniform(splits[4], (4, NFLAT, FLON), jnp.float32) ** block_scale(splits[4], (4, NFLAT, FLON), ((1, 64),), -0.2, 0.2), 0.1, 0.5),
        "obs_mask": set_ends((jax.random.randint(splits[5], (NT, NFLAT, FLON), 0, 2) < 1).astype(jnp.int32), jax.random.fold_in(splits[5], 1), 0, 1),
        "innovation": scatter_about(splits[6], (NT, NFLAT, FLON), 2.0, 12.0, ((1, 64),), jnp.float32),
    }


C_MID = 0.5
C_SIDE = 0.25
STEP_SIZE = 0.5
HIGHEST_PRECISION = lax.Precision.HIGHEST


def lon_filter(source_field, widths):
    scaled = 1.0 / (2.0 * widths.astype(jnp.float32) + 1.0)
    summed = jnp.zeros_like(source_field)
    for offset in range(-WIDEST, WIDEST + 1):
        weight_row = jnp.where(abs(offset) <= widths, scaled, 0.0 * scaled)
        summed = summed + jnp.roll(source_field, offset, axis=-1) * weight_row[:, None]
    return summed


def lat_filter(source_field):
    padded = jnp.pad(source_field, ((0, 0), (1, 1), (0, 0)))
    return C_MID * source_field + C_SIDE * (padded[:, :-2] + padded[:, 2:])


def obs_stencil(fine_field):
    return 0.25 * jnp.roll(fine_field, 1, axis=-1) + 0.5 * fine_field + 0.25 * jnp.roll(fine_field, -1, axis=-1)


def reference(control, ensemble, widths, interp_source, interp_weight, obs_mask, innovation):
    band_index = jnp.arange(NFLAT, dtype=jnp.int32) // (2 * CLAT)
    band_offset = (band_index * (CLAT * NLON)).astype(jnp.int32)[None, :, None]
    flat_source = (interp_source + band_offset).astype(jnp.int32).reshape(-1)
    obs_weight = obs_mask.astype(jnp.float32)
    control_now = control
    for iteration in range(GRAD_STEPS):
        forward = lat_filter(lon_filter(control_now, widths))
        coarse = jnp.einsum("mtri,mri->tri", ensemble, forward, precision=HIGHEST_PRECISION)
        padded = jnp.pad(coarse, ((0, 0), (1, 1), (0, 0))).reshape(NT, -1)
        picked = jnp.take(padded, flat_source, axis=1).reshape((NT,) + interp_weight.shape)
        fine_field = jnp.sum(picked * interp_weight[None], axis=1)
        misfit = obs_weight * (obs_stencil(fine_field) - innovation)
        fine_grid_return = obs_stencil(misfit)
        spread = (fine_grid_return[:, None] * interp_weight[None]).reshape(NT, -1)
        landed = jnp.zeros((NT, (NLAT + 2) * NLON), jnp.float32).at[:, flat_source].add(spread)
        coarse_back = landed.reshape(NT, NLAT + 2, NLON)[:, 1:-1]
        member_back = jnp.einsum("mtri,tri->mri", ensemble, coarse_back, precision=HIGHEST_PRECISION)
        gradient = control_now + lon_filter(lat_filter(member_back), widths)
        control_now = control_now - STEP_SIZE * gradient
    return control_now
```

```python
import jax
import jax.numpy as jnp
from jax import lax
from jax.experimental import pallas as pl
from jax.experimental.pallas import tpu as pltpu
from jax.sharding import PartitionSpec as P

WIDEST = 4
STEP_SIZE = 0.5
C_MID = 0.5
C_SIDE = 0.25

F32 = jnp.float32
LIMIT = 40 * 1024 * 1024


def shape(*dims):
    return jax.ShapeDtypeStruct(dims, F32)


def call(kernel, outs, args, scalars=(), flops=1_000_000):
    in_specs = [pl.BlockSpec(memory_space=pltpu.SMEM)] * len(scalars)
    in_specs += [pl.BlockSpec(memory_space=pltpu.VMEM)] * len(args)
    args = tuple(scalars) + tuple(args)
    return pl.pallas_call(
        kernel,
        out_shape=outs,
        in_specs=in_specs,
        out_specs=jax.tree.map(lambda _: pl.BlockSpec(memory_space=pltpu.VMEM), outs),
        compiler_params=pltpu.CompilerParams(vmem_limit_bytes=LIMIT),
        cost_estimate=pl.CostEstimate(flops=flops, transcendentals=0, bytes_accessed=1_000_000),
    )(*args)


def iota(shape_, dim):
    return lax.broadcasted_iota(jnp.int32, shape_, dim)


def shifted(x, k):
    nd = x.ndim
    turned = pltpu.roll(x, k % 128, nd - 1)
    lane = iota(x.shape, nd - 1)
    if k > 0:
        return jnp.where(lane < k, pltpu.roll(turned, 1, nd - 2), turned)
    return jnp.where(lane >= 128 + k, pltpu.roll(turned, 7, nd - 2), turned)


def tap_weights(widths_ref, r):
    width = jnp.full((8, 128), widths_ref[r], jnp.int32)
    scaled = 1.0 / (2.0 * width.astype(F32) + 1.0)
    return [jnp.where(k <= width, scaled, 0.0) for k in range(WIDEST + 1)]


def if_inside(place_ref, above, below):
    band = jnp.full((8, 128), place_ref[0], jnp.int32)
    last = jnp.full((8, 128), place_ref[1], jnp.int32)
    return jnp.where(band > 0, above, 0.0), jnp.where(band < last, below, 0.0)


def lon_filter(x, taps):
    total = x * taps[0]
    for k in range(1, WIDEST + 1):
        total = total + (shifted(x, k) + shifted(x, -k)) * taps[k]
    return total


def filter_kernel(widths_ref, v_ref, w0_ref, w1_ref):
    for r, out in ((0, w0_ref), (1, w1_ref)):
        taps = tap_weights(widths_ref, r)

        def body(b, carry, r=r, out=out, taps=taps):
            x = v_ref[pl.ds(b * 4, 4), pl.ds(r, 8, stride=2), :]
            out[pl.ds(b * 4, 4)] = lon_filter(x, taps)
            return carry

        lax.fori_loop(0, 8, body, 0)


def split_kernel(e_ref, e0_ref, e1_ref):
    def body(b, carry):
        at = pl.ds(b * 8, 8)
        e0_ref[at] = e_ref[at, pl.ds(0, 8, stride=2), :]
        e1_ref[at] = e_ref[at, pl.ds(1, 8, stride=2), :]
        return carry

    lax.fori_loop(0, 16, body, 0)


def planes_kernel(src_ref, wgt_ref, msk_ref, inn_ref, planes_ref, mask_ref, target_ref):
    parent = iota((8, 128), 0) * 128 + iota((8, 128), 1) // 2
    for j in range(8):
        half, fr = j // 4, j % 4
        at = pl.ds(j, 8, stride=8)
        codes, weights = [], []
        for s in range(4):
            src = src_ref[s, at, :]
            row_shift = lax.shift_right_logical(src, 10) - (fr // 2 + 1)
            col = jnp.bitwise_and(src, 1023)
            col_shift = jnp.bitwise_and(col - parent - half * 64 + 2, 1023) - 2
            codes.append((row_shift + 1) * 5 + col_shift + 2)
            weights.append(wgt_ref[s, at, :])
        for n in range(15):
            total = jnp.where(codes[0] == n, weights[0], 0.0)
            for s in range(1, 4):
                total = total + jnp.where(codes[s] == n, weights[s], 0.0)
            planes_ref[n, j] = total
        for t in range(4):
            mask_ref[t, j] = msk_ref[t, at, :].astype(F32)
            target_ref[t, j] = inn_ref[t, at, :]


def first_kernel(place_ref, w0_ref, w1_ref, above_ref, below_ref, e0_ref, e1_ref, part_ref):
    def body(m, sums):
        a, b = w0_ref[m], w1_ref[m]
        above, below = if_inside(place_ref, above_ref[m], below_ref[m])
        f0 = C_MID * a + C_SIDE * (above + b)
        f1 = C_MID * b + C_SIDE * (a + below)
        sums = list(sums)
        for t in range(4):
            sums[t] = sums[t] + e0_ref[m * 4 + t] * f0
            sums[4 + t] = sums[4 + t] + e1_ref[m * 4 + t] * f1
        return tuple(sums)

    sums = lax.fori_loop(0, 32, body, (jnp.zeros((8, 128), F32),) * 8, unroll=4)
    for n in range(8):
        part_ref[n] = sums[n]


def sum_kernel(parts_ref, a_ref, b_ref):
    count = a_ref.shape[0]
    for n in range(2 * count):
        total = (parts_ref[0, n] + parts_ref[1, n]) + (parts_ref[2, n] + parts_ref[3, n])
        if n < count:
            a_ref[n] = total
        else:
            b_ref[n - count] = total


def lanes(x, index):
    return jnp.take_along_axis(x, index, axis=1)


def stencil(a, b):
    lane = iota((8, 128), 1)
    a1, b1 = pltpu.roll(a, 1, 1), pltpu.roll(b, 1, 1)
    left_a = jnp.where(lane == 0, pltpu.roll(b1, 1, 0), a1)
    left_b = jnp.where(lane == 0, a1, b1)
    a2, b2 = pltpu.roll(a, 127, 1), pltpu.roll(b, 127, 1)
    right_a = jnp.where(lane == 127, b2, a2)
    right_b = jnp.where(lane == 127, pltpu.roll(a2, 7, 0), b2)
    return 0.5 * a + 0.25 * (left_a + right_a), 0.5 * b + 0.25 * (left_b + right_b)


def observe_slot(t, rows, planes_ref, mask_ref, target_ref):
    lane = iota((8, 128), 1)
    up = [lane // 2, lane // 2 + 64]
    down = jnp.bitwise_and(lane * 2, 127)
    fine = [None] * 8
    for q in range(4):
        for d in range(-2, 3):
            x = rows[q] if d == 0 else shifted(rows[q], -d)
            for half in range(2):
                u = lanes(x, up[half])
                for fr in range(4):
                    rs = q - 1 - fr // 2
                    if -1 <= rs <= 1:
                        j = half * 4 + fr
                        term = planes_ref[(rs + 1) * 5 + d + 2, j] * u
                        fine[j] = term if fine[j] is None else fine[j] + term
    back = [None] * 8
    for fr in range(4):
        a, b = stencil(fine[fr], fine[4 + fr])
        a = mask_ref[t, fr] * (a - target_ref[t, fr])
        b = mask_ref[t, 4 + fr] * (b - target_ref[t, 4 + fr])
        back[fr], back[4 + fr] = stencil(a, b)
    landed = []
    for q in range(4):
        total = None
        for d in range(-2, 3):
            halves = []
            for half in range(2):
                z = None
                for fr in range(4):
                    rs = q - 1 - fr // 2
                    if -1 <= rs <= 1:
                        j = half * 4 + fr
                        term = planes_ref[(rs + 1) * 5 + d + 2, j] * back[j]
                        z = term if z is None else z + term
                z = z + pltpu.roll(z, 127, 1)
                halves.append(lanes(z, down))
            w = jnp.where(lane < 64, halves[0], halves[1])
            w = w if d == 0 else shifted(w, d)
            total = w if total is None else total + w
        landed.append(total)
    return landed


def first_observe_kernel(above_ref, c0_ref, c1_ref, below_ref, planes_ref, mask_ref, target_ref, la_ref, lb_ref):
    for t in range(4):
        rows = [above_ref[t], c0_ref[t], c1_ref[t], below_ref[t]]
        landed = observe_slot(t, rows, planes_ref, mask_ref, target_ref)
        la_ref[t], la_ref[4 + t], lb_ref[t], lb_ref[4 + t] = landed


def second_observe_kernel(ca_ref, cb_ref, da_ref, db_ref, planes_ref, mask_ref, target_ref, la_ref, lb_ref):
    for t in range(4):
        rows = [
            ca_ref[t] + da_ref[t],
            ca_ref[4 + t] + da_ref[4 + t],
            cb_ref[t] + db_ref[t],
            cb_ref[4 + t] + db_ref[4 + t],
        ]
        landed = observe_slot(t, rows, planes_ref, mask_ref, target_ref)
        la_ref[t], la_ref[4 + t], lb_ref[t], lb_ref[4 + t] = landed


def member_back(e_ref, at, weights):
    x = e_ref[pl.ds(at * 16, 16)].reshape(4, 4, 8, 128)
    total = x[:, 0] * weights[0]
    for t in range(1, 4):
        total = total + x[:, t] * weights[t]
    return total


def adjoint_rows(place_ref, la_ref, lb_ref, ra_ref, rb_ref):
    rows = []
    for mine, theirs in ((la_ref, ra_ref), (lb_ref, rb_ref)):
        for half in range(2):
            rows.append([mine[half * 4 + t] + theirs[half * 4 + t] for t in range(4)])
    for t in range(4):
        rows[0][t], rows[3][t] = if_inside(place_ref, rows[0][t], rows[3][t])
    return rows


def descend(b, e_refs, rows, old, taps):
    back = [member_back(e_refs[q], b, rows[q]) for q in range(4)]
    fresh = []
    for r in range(2):
        smooth = C_MID * back[r + 1] + C_SIDE * (back[r] + back[r + 2])
        gradient = old[r] + lon_filter(smooth, taps[r])
        fresh.append(old[r] - STEP_SIZE * gradient)
    return fresh


def middle_kernel(widths_ref, place_ref, la_ref, lb_ref, ra_ref, rb_ref, em_ref, e0_ref, e1_ref, ep_ref, v_ref, new_ref, part_ref):
    rows = adjoint_rows(place_ref, la_ref, lb_ref, ra_ref, rb_ref)
    taps = [tap_weights(widths_ref, r) for r in range(2)]
    e_refs = (em_ref, e0_ref, e1_ref, ep_ref)
    part_ref[...] = jnp.zeros_like(part_ref)

    def body(b, carry):
        at = pl.ds(b * 4, 4)
        old = [v_ref[at, pl.ds(r, 8, stride=2), :] for r in range(2)]
        fresh = descend(b, e_refs, rows, old, taps)
        for r in range(2):
            new_ref[r, at] = fresh[r]
        w = [lon_filter(fresh[r], taps[r]) for r in range(2)]
        forward = [
            C_SIDE * w[0],
            C_MID * w[0] + C_SIDE * w[1],
            C_MID * w[1] + C_SIDE * w[0],
            C_SIDE * w[1],
        ]
        forward[0], forward[3] = if_inside(place_ref, forward[0], forward[3])
        for q in range(4):
            x = e_refs[q][pl.ds(b * 16, 16)].reshape(4, 4, 8, 128)
            for t in range(4):
                part_ref[q * 4 + t] += jnp.sum(x[:, t] * forward[q], axis=0)
        return carry

    lax.fori_loop(0, 8, body, 0)


def last_kernel(widths_ref, place_ref, la_ref, lb_ref, ra_ref, rb_ref, em_ref, e0_ref, e1_ref, ep_ref, v_ref, out_ref):
    rows = adjoint_rows(place_ref, la_ref, lb_ref, ra_ref, rb_ref)
    taps = [tap_weights(widths_ref, r) for r in range(2)]
    e_refs = (em_ref, e0_ref, e1_ref, ep_ref)

    def body(b, carry):
        at = pl.ds(b * 4, 4)
        old = [v_ref[r, at] for r in range(2)]
        fresh = descend(b, e_refs, rows, old, taps)
        for r in range(2):
            out_ref[at, pl.ds(r, 8, stride=2), :] = fresh[r]
        return carry

    lax.fori_loop(0, 8, body, 0)


def to_next(x):
    count = lax.axis_size("lat")
    return lax.ppermute(x, "lat", [(i, (i + 1) % count) for i in range(count)])


def to_previous(x):
    count = lax.axis_size("lat")
    return lax.ppermute(x, "lat", [((i + 1) % count, i) for i in range(count)])


def tiles(x):
    lead, (rows, cols) = x.shape[:-2], x.shape[-2:]
    x = x.reshape(-1, rows, cols // 128, 128).transpose(0, 2, 1, 3)
    return x.reshape(-1, cols // 128 * rows, 128)


def local(control, ensemble, widths, interp_source, interp_weight, obs_mask, innovation):
    v = tiles(control)
    e = tiles(ensemble)
    place = jnp.stack([lax.axis_index("lat"), lax.axis_size("lat") - 1]).astype(jnp.int32)
    row = shape(32, 8, 128)
    w0, w1 = call(filter_kernel, (row, row), (v,), (widths,))
    above, below = to_next(w1), to_previous(w0)
    e0, e1 = call(split_kernel, (shape(128, 8, 128),) * 2, (e,))
    e_above, e_below = to_next(e1), to_previous(e0)
    fields = call(
        planes_kernel,
        (shape(15, 8, 8, 128), shape(4, 8, 8, 128), shape(4, 8, 8, 128)),
        tuple(tiles(x) for x in (interp_source, interp_weight, obs_mask, innovation)),
    )
    part = call(first_kernel, shape(8, 8, 128), (w0, w1, above, below, e0, e1), (place,))
    four, eight = shape(4, 8, 128), shape(8, 8, 128)
    c0, c1 = call(sum_kernel, (four, four), (lax.all_gather(part, "mem"),))
    la, lb = call(
        first_observe_kernel, (eight, eight), (to_next(c1), c0, c1, to_previous(c0)) + tuple(fields)
    )
    ra, rb = to_next(lb), to_previous(la)
    new, part = call(
        middle_kernel,
        (shape(2, 32, 8, 128), shape(16, 8, 128)),
        (la, lb, ra, rb, e_above, e0, e1, e_below, v),
        (widths, place),
    )
    ca, cb = call(sum_kernel, (eight, eight), (lax.all_gather(part, "mem"),))
    la, lb = call(
        second_observe_kernel, (eight, eight), (ca, cb, to_next(cb), to_previous(ca)) + tuple(fields)
    )
    ra, rb = to_next(lb), to_previous(la)
    out = call(
        last_kernel,
        shape(32, 16, 128),
        (la, lb, ra, rb, e_above, e0, e1, e_below, new),
        (widths, place),
    )
    return out.reshape(32, 8, 2, 128).transpose(0, 2, 1, 3).reshape(control.shape)


def solution(mesh):
    in_specs = (
        P("mem", "lat", None),
        P("mem", None, "lat", None),
        P("lat"),
        P(None, "lat", None),
        P(None, "lat", None),
        P(None, "lat", None),
        P(None, "lat", None),
    )
    out_specs = P("mem", "lat", None)
    return jax.shard_map(local, mesh=mesh, in_specs=in_specs, out_specs=out_specs, check_vma=False)
```

```python
import jax
import jax.numpy as jnp
from jax import lax
from jax.experimental import pallas as pl
from jax.experimental.pallas import tpu as pltpu
from jax.sharding import PartitionSpec as P

STEP_SIZE = 0.5
C_MID = 0.5
C_SIDE = 0.25

F32 = jnp.float32
LIMIT = 40 * 1024 * 1024


def shape(*dims):
    return jax.ShapeDtypeStruct(dims, F32)


def call(kernel, outs, args, scalars=(), scratch=(), flops=1_000_000):
    in_specs = [pl.BlockSpec(memory_space=pltpu.SMEM)] * len(scalars)
    in_specs += [pl.BlockSpec(memory_space=pltpu.VMEM)] * len(args)
    args = tuple(scalars) + tuple(args)
    return pl.pallas_call(
        kernel,
        out_shape=outs,
        in_specs=in_specs,
        out_specs=jax.tree.map(lambda _: pl.BlockSpec(memory_space=pltpu.VMEM), outs),
        scratch_shapes=[pltpu.VMEM(dims, F32) for dims in scratch],
        compiler_params=pltpu.CompilerParams(vmem_limit_bytes=LIMIT),
        cost_estimate=pl.CostEstimate(flops=flops, transcendentals=0, bytes_accessed=1_000_000),
    )(*args)


def iota(shape_, dim):
    return lax.broadcasted_iota(jnp.int32, shape_, dim)


def position(k):
    return jnp.where(k < 128, k, jnp.where(k < 192, k, k - 256))


def widened(x):
    n = x.shape[0]
    y = jnp.where(iota(x.shape, 2) < 64, pltpu.roll(x, 7, 1), pltpu.roll(x, 1, 1))
    return jnp.concatenate([x.reshape(n * 8, 128), y.reshape(n * 8, 128)], axis=1)


def product(x, matrix):
    high = x.astype(jnp.bfloat16)
    rest = x - high.astype(F32)
    middle = rest.astype(jnp.bfloat16)
    low = (rest - middle.astype(F32)).astype(jnp.bfloat16)
    total = jnp.dot(low, matrix, preferred_element_type=F32)
    total = total + jnp.dot(middle, matrix, preferred_element_type=F32)
    return total + jnp.dot(high, matrix, preferred_element_type=F32)


def filtered(x, band, scale):
    return product(widened(x), band).reshape(x.shape) * scale


def scale_of(widths_ref, r):
    width = jnp.full((8, 128), widths_ref[r], jnp.int32)
    return 1.0 / (2.0 * width.astype(F32) + 1.0)


def if_inside(place_ref, above, below):
    band = jnp.full((8, 128), place_ref[0], jnp.int32)
    last = jnp.full((8, 128), place_ref[1], jnp.int32)
    return jnp.where(band > 0, above, 0.0), jnp.where(band < last, below, 0.0)


def filter_kernel(widths_ref, v_ref, w0_ref, w1_ref, band_ref):
    away = jnp.abs(position(iota((256, 128), 0)) - iota((256, 128), 1))
    for r, out in ((0, w0_ref), (1, w1_ref)):
        inside = away <= jnp.full((256, 128), widths_ref[r], jnp.int32)
        band = jnp.where(inside, 1.0, 0.0).astype(jnp.bfloat16)
        band_ref[r] = band
        scale = scale_of(widths_ref, r)
        for b in range(2):
            x = v_ref[pl.ds(b * 16, 16), pl.ds(r, 8, stride=2), :]
            out[pl.ds(b * 16, 16)] = filtered(x, band, scale)


def split_kernel(e_ref, e0_ref, e1_ref):
    def body(b, carry):
        at = pl.ds(b * 8, 8)
        e0_ref[at] = e_ref[at, pl.ds(0, 8, stride=2), :]
        e1_ref[at] = e_ref[at, pl.ds(1, 8, stride=2), :]
        return carry

    lax.fori_loop(0, 16, body, 0)


def planes_kernel(src_ref, wgt_ref, msk_ref, inn_ref, planes_ref, mask_ref, target_ref, refine_ref, gather_ref):
    parent = iota((8, 128), 0) * 128 + iota((8, 128), 1) // 2
    for j in range(8):
        half, fr = j // 4, j % 4
        at = pl.ds(j, 8, stride=8)
        codes, weights = [], []
        for s in range(4):
            src = src_ref[s, at, :]
            row_shift = lax.shift_right_logical(src, 10) - (fr // 2 + 1)
            col = jnp.bitwise_and(src, 1023)
            col_shift = jnp.bitwise_and(col - parent - half * 64 + 2, 1023) - 2
            codes.append((row_shift + 1) * 5 + col_shift + 2)
            weights.append(wgt_ref[s, at, :])
        for n in range(15):
            total = jnp.where(codes[0] == n, weights[0], 0.0)
            for s in range(1, 4):
                total = total + jnp.where(codes[s] == n, weights[s], 0.0)
            planes_ref[n, j] = total
        for t in range(4):
            mask_ref[t, j] = msk_ref[t, at, :].astype(F32)
            target_ref[t, j] = inn_ref[t, at, :]
    for n in range(10):
        d, half = n // 2 - 2, n % 2
        source = half * 64 + iota((256, 128), 1) // 2 + d
        hit = position(iota((256, 128), 0)) == source
        refine_ref[:, n * 128 : n * 128 + 128] = jnp.where(hit, 1.0, 0.0).astype(jnp.bfloat16)
        source = half * 64 + iota((128, 256), 0) // 2 + d
        hit = position(iota((128, 256), 1)) == source
        gather_ref[n * 128 : n * 128 + 128, :] = jnp.where(hit, 1.0, 0.0).astype(jnp.bfloat16)


def first_kernel(place_ref, w0_ref, w1_ref, above_ref, below_ref, e0_ref, e1_ref, part_ref):
    def body(m, sums):
        a, b = w0_ref[m], w1_ref[m]
        above, below = if_inside(place_ref, above_ref[m], below_ref[m])
        f0 = C_MID * a + C_SIDE * (above + b)
        f1 = C_MID * b + C_SIDE * (a + below)
        sums = list(sums)
        for t in range(4):
            sums[t] = sums[t] + e0_ref[m * 4 + t] * f0
            sums[4 + t] = sums[4 + t] + e1_ref[m * 4 + t] * f1
        return tuple(sums)

    sums = lax.fori_loop(0, 32, body, (jnp.zeros((8, 128), F32),) * 8, unroll=4)
    for n in range(8):
        part_ref[n] = sums[n]


def sum_kernel(parts_ref, a_ref, b_ref):
    count = a_ref.shape[0]
    for n in range(2 * count):
        total = (parts_ref[0, n] + parts_ref[1, n]) + (parts_ref[2, n] + parts_ref[3, n])
        if n < count:
            a_ref[n] = total
        else:
            b_ref[n - count] = total


def stencil(a, b):
    lane = iota((8, 128), 1)
    a1, b1 = pltpu.roll(a, 1, 1), pltpu.roll(b, 1, 1)
    left_a = jnp.where(lane == 0, pltpu.roll(b1, 1, 0), a1)
    left_b = jnp.where(lane == 0, a1, b1)
    a2, b2 = pltpu.roll(a, 127, 1), pltpu.roll(b, 127, 1)
    right_a = jnp.where(lane == 127, b2, a2)
    right_b = jnp.where(lane == 127, pltpu.roll(a2, 7, 0), b2)
    return 0.5 * a + 0.25 * (left_a + right_a), 0.5 * b + 0.25 * (left_b + right_b)


def observe(rows, planes_ref, mask_ref, target_ref, refine_ref, gather_ref, u_ref, la_ref, lb_ref):
    window = jnp.stack([rows[t][q] for t in range(4) for q in range(4)])
    u_ref[...] = product(widened(window), refine_ref[...])

    def piece(t, q, d, half):
        n = d * 2 + half
        return u_ref[pl.ds((t * 4 + q) * 8, 8), pl.ds(n * 128, 128)]

    back = {}
    for r in range(2):
        fine = {}
        for half in range(2):
            for rs in range(-1, 2):
                for d in range(5):
                    u = [piece(t, r + 1 + rs, d, half) for t in range(4)]
                    for fr in (2 * r, 2 * r + 1):
                        plane = planes_ref[(rs + 1) * 5 + d, half * 4 + fr]
                        for t in range(4):
                            key = (t, fr, half)
                            fine[key] = fine[key] + plane * u[t] if key in fine else plane * u[t]
        for t in range(4):
            for fr in (2 * r, 2 * r + 1):
                pair = stencil(fine[t, fr, 0], fine[t, fr, 1])
                pair = [
                    mask_ref[t, half * 4 + fr] * (pair[half] - target_ref[t, half * 4 + fr])
                    for half in range(2)
                ]
                back[t, fr, 0], back[t, fr, 1] = stencil(*pair)
    for half in range(2):
        for d in range(5):
            n = d * 2 + half
            for q in range(4):
                z = [None] * 4
                for fr in range(4):
                    rs = q - 1 - fr // 2
                    if -1 <= rs <= 1:
                        plane = planes_ref[(rs + 1) * 5 + d, half * 4 + fr]
                        for t in range(4):
                            term = plane * back[t, fr, half]
                            z[t] = term if z[t] is None else z[t] + term
                for t in range(4):
                    u_ref[pl.ds((t * 4 + q) * 8, 8), pl.ds(n * 128, 128)] = z[t]
    total = None
    for d in range(5):
        term = product(u_ref[:, d * 256 : d * 256 + 256], gather_ref[d * 256 : d * 256 + 256, :])
        total = term if total is None else total + term
    own, beside = total[:, :128].reshape(16, 8, 128), total[:, 128:].reshape(16, 8, 128)
    head = iota((16, 8, 128), 2) < 64
    landed = own + jnp.where(head, pltpu.roll(beside, 1, 1), pltpu.roll(beside, 7, 1))
    for t in range(4):
        la_ref[t], la_ref[4 + t] = landed[t * 4], landed[t * 4 + 1]
        lb_ref[t], lb_ref[4 + t] = landed[t * 4 + 2], landed[t * 4 + 3]


def first_observe_kernel(above_ref, c0_ref, c1_ref, below_ref, *refs):
    observe([[ref[t] for ref in (above_ref, c0_ref, c1_ref, below_ref)] for t in range(4)], *order(refs))


def second_observe_kernel(ca_ref, cb_ref, da_ref, db_ref, *refs):
    rows = [
        [
            mine[half * 4 + t] + theirs[half * 4 + t]
            for mine, theirs in ((ca_ref, da_ref), (cb_ref, db_ref))
            for half in range(2)
        ]
        for t in range(4)
    ]
    observe(rows, *order(refs))


def order(refs):
    *fields, la_ref, lb_ref, u_ref = refs
    return *fields, u_ref, la_ref, lb_ref


def adjoint_rows(place_ref, la_ref, lb_ref, ra_ref, rb_ref):
    rows = []
    for mine, theirs in ((la_ref, ra_ref), (lb_ref, rb_ref)):
        for half in range(2):
            rows.append([mine[half * 4 + t] + theirs[half * 4 + t] for t in range(4)])
    for t in range(4):
        rows[0][t], rows[3][t] = if_inside(place_ref, rows[0][t], rows[3][t])
    return rows


def smoothed_back(e_refs, rows, s_ref):
    def body(b, carry):
        back = []
        for q in range(4):
            x = e_refs[q][pl.ds(b * 16, 16)].reshape(4, 4, 8, 128)
            total = x[:, 0] * rows[q][0]
            for t in range(1, 4):
                total = total + x[:, t] * rows[q][t]
            back.append(total)
        for r in range(2):
            s_ref[r, pl.ds(b * 4, 4)] = C_MID * back[r + 1] + C_SIDE * (back[r] + back[r + 2])
        return carry

    lax.fori_loop(0, 8, body, 0, unroll=2)


def middle_kernel(
    widths_ref, place_ref, la_ref, lb_ref, ra_ref, rb_ref, em_ref, e0_ref, e1_ref, ep_ref,
    band_ref, v_ref, new_ref, part_ref, s_ref,
):
    rows = adjoint_rows(place_ref, la_ref, lb_ref, ra_ref, rb_ref)
    e_refs = (em_ref, e0_ref, e1_ref, ep_ref)
    smoothed_back(e_refs, rows, s_ref)
    for r in range(2):
        scale = scale_of(widths_ref, r)
        for b in range(2):
            at = pl.ds(b * 16, 16)
            old = v_ref[at, pl.ds(r, 8, stride=2), :]
            gradient = old + filtered(s_ref[r, at], band_ref[r], scale)
            new = old - STEP_SIZE * gradient
            new_ref[r, at] = new
            s_ref[r, at] = filtered(new, band_ref[r], scale)

    def body(b, sums):
        sums = list(sums)
        for i in range(4):
            m = b * 4 + i
            w = [s_ref[r, m] for r in range(2)]
            forward = [
                C_SIDE * w[0],
                C_MID * w[0] + C_SIDE * w[1],
                C_MID * w[1] + C_SIDE * w[0],
                C_SIDE * w[1],
            ]
            for q in range(4):
                for t in range(4):
                    sums[q * 4 + t] = sums[q * 4 + t] + e_refs[q][m * 4 + t] * forward[q]
        return tuple(sums)

    sums = list(lax.fori_loop(0, 8, body, (jnp.zeros((8, 128), F32),) * 16))
    for t in range(4):
        sums[t], sums[12 + t] = if_inside(place_ref, sums[t], sums[12 + t])
    for n in range(16):
        part_ref[n] = sums[n]


def last_kernel(
    widths_ref, place_ref, la_ref, lb_ref, ra_ref, rb_ref, em_ref, e0_ref, e1_ref, ep_ref,
    band_ref, v_ref, out_ref, s_ref,
):
    rows = adjoint_rows(place_ref, la_ref, lb_ref, ra_ref, rb_ref)
    smoothed_back((em_ref, e0_ref, e1_ref, ep_ref), rows, s_ref)
    for r in range(2):
        scale = scale_of(widths_ref, r)
        for b in range(2):
            at = pl.ds(b * 16, 16)
            old = v_ref[r, at]
            gradient = old + filtered(s_ref[r, at], band_ref[r], scale)
            out_ref[at, pl.ds(r, 8, stride=2), :] = old - STEP_SIZE * gradient


def ring(step):
    groups, bands = lax.axis_size("mem"), lax.axis_size("lat")
    pairs = []
    for m in range(groups):
        for i in range(bands):
            inside = 0 <= i + step < bands
            other = m if inside else (m + groups // 2) % groups
            pairs.append((m * bands + i, other * bands + (i + step) % bands))
    return pairs


def to_next(x):
    return lax.ppermute(x, ("mem", "lat"), ring(1))


def to_previous(x):
    return lax.ppermute(x, ("mem", "lat"), ring(-1))


def tiles(x):
    (rows, cols) = x.shape[-2:]
    x = x.reshape(-1, rows, cols // 128, 128).transpose(0, 2, 1, 3)
    return x.reshape(-1, cols // 128 * rows, 128)


def descent(control, ensemble, widths, interp_source, interp_weight, obs_mask, innovation):
    v = tiles(control)
    e = tiles(ensemble)
    place = jnp.stack([lax.axis_index("lat"), lax.axis_size("lat") - 1]).astype(jnp.int32)
    row = shape(32, 8, 128)
    band = jax.ShapeDtypeStruct((2, 256, 128), jnp.bfloat16)
    w0, w1, band = call(filter_kernel, (row, row, band), (v,), (widths,))
    above, below = to_next(w1), to_previous(w0)
    e, w0, w1 = lax.optimization_barrier((e, w0, w1))
    e0, e1 = call(split_kernel, (shape(128, 8, 128),) * 2, (e,))
    e_above, e_below = to_next(e1), to_previous(e0)
    fields = call(
        planes_kernel,
        (
            shape(15, 8, 8, 128),
            shape(4, 8, 8, 128),
            shape(4, 8, 8, 128),
            jax.ShapeDtypeStruct((256, 1280), jnp.bfloat16),
            jax.ShapeDtypeStruct((1280, 256), jnp.bfloat16),
        ),
        tuple(tiles(x) for x in (interp_source, interp_weight, obs_mask, innovation)),
    )
    part = call(first_kernel, shape(8, 8, 128), (w0, w1, above, below, e0, e1), (place,))
    four, eight = shape(4, 8, 128), shape(8, 8, 128)
    c0, c1 = call(sum_kernel, (four, four), (lax.all_gather(part, "mem"),))
    refined = ((128, 1280),)
    la, lb = call(
        first_observe_kernel,
        (eight, eight),
        (to_next(c1), c0, c1, to_previous(c0)) + tuple(fields),
        scratch=refined,
    )
    ra, rb = to_next(lb), to_previous(la)
    ensembles = (e_above, e0, e1, e_below, band)
    smoothed = ((2, 32, 8, 128),)
    new, part = call(
        middle_kernel,
        (shape(2, 32, 8, 128), shape(16, 8, 128)),
        (la, lb, ra, rb) + ensembles + (v,),
        (widths, place),
        smoothed,
    )
    ca, cb = call(sum_kernel, (eight, eight), (lax.all_gather(part, "mem"),))
    la, lb = call(
        second_observe_kernel,
        (eight, eight),
        (ca, cb, to_next(cb), to_previous(ca)) + tuple(fields),
        scratch=refined,
    )
    ra, rb = to_next(lb), to_previous(la)
    out = call(
        last_kernel,
        shape(32, 16, 128),
        (la, lb, ra, rb) + ensembles + (new,),
        (widths, place),
        smoothed,
    )
    return out.reshape(32, 8, 2, 128).transpose(0, 2, 1, 3).reshape(control.shape)


def solution(mesh):
    in_specs = (
        P("mem", "lat", None),
        P("mem", None, "lat", None),
        P("lat"),
        P(None, "lat", None),
        P(None, "lat", None),
        P(None, "lat", None),
        P(None, "lat", None),
    )
    out_specs = P("mem", "lat", None)
    return jax.shard_map(descent, mesh=mesh, in_specs=in_specs, out_specs=out_specs, check_vma=False)
```

```python
import jax
import jax.numpy as jnp
from jax import lax
from jax.experimental import pallas as pl
from jax.experimental.pallas import tpu as pltpu
from jax.sharding import PartitionSpec as P

STEP_SIZE = 0.5
C_MID = 0.5
C_SIDE = 0.25

F32 = jnp.float32
LIMIT = 40 * 1024 * 1024


def shape(*dims):
    return jax.ShapeDtypeStruct(dims, F32)


def call(kernel, outs, args, scalars=(), scratch=(), flops=1_000_000):
    in_specs = [pl.BlockSpec(memory_space=pltpu.SMEM)] * len(scalars)
    in_specs += [pl.BlockSpec(memory_space=pltpu.VMEM)] * len(args)
    args = tuple(scalars) + tuple(args)
    return pl.pallas_call(
        kernel,
        out_shape=outs,
        in_specs=in_specs,
        out_specs=jax.tree.map(lambda _: pl.BlockSpec(memory_space=pltpu.VMEM), outs),
        scratch_shapes=[pltpu.VMEM(dims, F32) for dims in scratch],
        compiler_params=pltpu.CompilerParams(vmem_limit_bytes=LIMIT),
        cost_estimate=pl.CostEstimate(flops=flops, transcendentals=0, bytes_accessed=1_000_000),
    )(*args)


def iota(shape_, dim):
    return lax.broadcasted_iota(jnp.int32, shape_, dim)


def position(k):
    return jnp.where(k < 128, k, jnp.where(k < 192, k, k - 256))


def widened(x):
    n = x.shape[0]
    y = jnp.where(iota(x.shape, 2) < 64, pltpu.roll(x, 7, 1), pltpu.roll(x, 1, 1))
    return jnp.concatenate([x.reshape(n * 8, 128), y.reshape(n * 8, 128)], axis=1)


def product(x, matrix):
    high = x.astype(jnp.bfloat16)
    rest = x - high.astype(F32)
    middle = rest.astype(jnp.bfloat16)
    low = (rest - middle.astype(F32)).astype(jnp.bfloat16)
    total = jnp.dot(low, matrix, preferred_element_type=F32)
    total = total + jnp.dot(middle, matrix, preferred_element_type=F32)
    return total + jnp.dot(high, matrix, preferred_element_type=F32)


def filtered(x, band, scale):
    return product(widened(x), band).reshape(x.shape) * scale


def width_of(widths_ref, place_ref, r):
    return widths_ref[r + place_ref[0] * (1 - 2 * r)]


def scale_of(width):
    return 1.0 / (2.0 * jnp.full((8, 128), width, jnp.int32).astype(F32) + 1.0)


def if_inside(place_ref, x):
    return jnp.where(jnp.full((8, 128), place_ref[1], jnp.int32) > 0, x, 0.0)


def if_odd(place_ref, odd, even):
    return jnp.where(jnp.full((8, 128), place_ref[0], jnp.int32) > 0, odd, even)


def filter_kernel(widths_ref, place_ref, v_ref, w0_ref, w1_ref, old_ref, band_ref):
    away = jnp.abs(position(iota((256, 128), 0)) - iota((256, 128), 1))
    for r, out in ((0, w0_ref), (1, w1_ref)):
        width = width_of(widths_ref, place_ref, r)
        inside = away <= jnp.full((256, 128), width, jnp.int32)
        band = jnp.where(inside, 1.0, 0.0).astype(jnp.bfloat16)
        band_ref[r] = band
        for b in range(2):
            at = pl.ds(b * 16, 16)
            top, bottom = (v_ref[at, pl.ds(n, 8, stride=2), :] for n in range(2))
            x = if_odd(place_ref, top, bottom) if r else if_odd(place_ref, bottom, top)
            old_ref[r, at] = x
            out[at] = filtered(x, band, scale_of(width))


def split_kernel(place_ref, e_ref, e0_ref, e1_ref):
    def body(b, carry):
        at = pl.ds(b * 8, 8)
        top, bottom = (e_ref[at, pl.ds(n, 8, stride=2), :] for n in range(2))
        e0_ref[at] = if_odd(place_ref, bottom, top)
        e1_ref[at] = if_odd(place_ref, top, bottom)
        return carry

    lax.fori_loop(0, 16, body, 0)


def planes_kernel(place_ref, src_ref, wgt_ref, msk_ref, inn_ref, planes_ref, mask_ref, target_ref, refine_ref, gather_ref):
    parent = iota((8, 128), 0) * 128 + iota((8, 128), 1) // 2
    odd = jnp.full((8, 128), place_ref[0], jnp.int32)
    for j in range(8):
        half, fr = j // 4, j % 4
        at, mirrored = pl.ds(j, 8, stride=8), pl.ds(half * 4 + 3 - fr, 8, stride=8)

        def row(ref, n, at=at, mirrored=mirrored):
            return jnp.where(odd > 0, ref[n, mirrored, :], ref[n, at, :])

        own_row = jnp.where(odd > 0, 1 - fr // 2, fr // 2)
        codes, weights = [], []
        for s in range(4):
            src = row(src_ref, s)
            row_shift = lax.shift_right_logical(src, 10) - (own_row + 1)
            row_shift = jnp.where(odd > 0, -row_shift, row_shift)
            col = jnp.bitwise_and(src, 1023)
            col_shift = jnp.bitwise_and(col - parent - half * 64 + 2, 1023) - 2
            codes.append((row_shift + 1) * 5 + col_shift + 2)
            weights.append(row(wgt_ref, s))
        for n in range(15):
            total = jnp.where(codes[0] == n, weights[0], 0.0)
            for s in range(1, 4):
                total = total + jnp.where(codes[s] == n, weights[s], 0.0)
            planes_ref[n, j] = total
        for t in range(4):
            mask_ref[t, j] = row(msk_ref, t).astype(F32)
            target_ref[t, j] = row(inn_ref, t)
    for n in range(10):
        d, half = n // 2 - 2, n % 2
        source = half * 64 + iota((256, 128), 1) // 2 + d
        hit = position(iota((256, 128), 0)) == source
        refine_ref[:, n * 128 : n * 128 + 128] = jnp.where(hit, 1.0, 0.0).astype(jnp.bfloat16)
        source = half * 64 + iota((128, 256), 0) // 2 + d
        hit = position(iota((128, 256), 1)) == source
        gather_ref[n * 128 : n * 128 + 128, :] = jnp.where(hit, 1.0, 0.0).astype(jnp.bfloat16)


def first_kernel(place_ref, w0_ref, w1_ref, far_ref, near_ref, e0_ref, e1_ref, part_ref):
    def body(m, sums):
        a, b = w0_ref[m], w1_ref[m]
        f0 = C_MID * a + C_SIDE * (if_inside(place_ref, far_ref[m]) + b)
        f1 = C_MID * b + C_SIDE * (a + near_ref[m])
        sums = list(sums)
        for t in range(4):
            sums[t] = sums[t] + e0_ref[m * 4 + t] * f0
            sums[4 + t] = sums[4 + t] + e1_ref[m * 4 + t] * f1
        return tuple(sums)

    sums = lax.fori_loop(0, 32, body, (jnp.zeros((8, 128), F32),) * 8, unroll=4)
    for n in range(8):
        part_ref[n] = sums[n]


def sum_kernel(parts_ref, a_ref, b_ref):
    count = a_ref.shape[0]
    for n in range(2 * count):
        total = (parts_ref[0, n] + parts_ref[1, n]) + (parts_ref[2, n] + parts_ref[3, n])
        if n < count:
            a_ref[n] = total
        else:
            b_ref[n - count] = total


def stencil(a, b):
    lane = iota((8, 128), 1)
    a1, b1 = pltpu.roll(a, 1, 1), pltpu.roll(b, 1, 1)
    left_a = jnp.where(lane == 0, pltpu.roll(b1, 1, 0), a1)
    left_b = jnp.where(lane == 0, a1, b1)
    a2, b2 = pltpu.roll(a, 127, 1), pltpu.roll(b, 127, 1)
    right_a = jnp.where(lane == 127, b2, a2)
    right_b = jnp.where(lane == 127, pltpu.roll(a2, 7, 0), b2)
    return 0.5 * a + 0.25 * (left_a + right_a), 0.5 * b + 0.25 * (left_b + right_b)


def observe(rows, planes_ref, mask_ref, target_ref, refine_ref, gather_ref, u_ref, far_ref, near_ref):
    window = jnp.stack([rows[t][q] for t in range(4) for q in range(4)])
    u_ref[...] = product(widened(window), refine_ref[...])

    def piece(t, q, d, half):
        n = d * 2 + half
        return u_ref[pl.ds((t * 4 + q) * 8, 8), pl.ds(n * 128, 128)]

    back = {}
    for r in range(2):
        fine = {}
        for half in range(2):
            for rs in range(-1, 2):
                for d in range(5):
                    u = [piece(t, r + 1 + rs, d, half) for t in range(4)]
                    for fr in (2 * r, 2 * r + 1):
                        plane = planes_ref[(rs + 1) * 5 + d, half * 4 + fr]
                        for t in range(4):
                            key = (t, fr, half)
                            fine[key] = fine[key] + plane * u[t] if key in fine else plane * u[t]
        for t in range(4):
            for fr in (2 * r, 2 * r + 1):
                pair = stencil(fine[t, fr, 0], fine[t, fr, 1])
                pair = [
                    mask_ref[t, half * 4 + fr] * (pair[half] - target_ref[t, half * 4 + fr])
                    for half in range(2)
                ]
                back[t, fr, 0], back[t, fr, 1] = stencil(*pair)
    for half in range(2):
        for d in range(5):
            n = d * 2 + half
            for q in range(4):
                z = [None] * 4
                for fr in range(4):
                    rs = q - 1 - fr // 2
                    if -1 <= rs <= 1:
                        plane = planes_ref[(rs + 1) * 5 + d, half * 4 + fr]
                        for t in range(4):
                            term = plane * back[t, fr, half]
                            z[t] = term if z[t] is None else z[t] + term
                for t in range(4):
                    u_ref[pl.ds((t * 4 + q) * 8, 8), pl.ds(n * 128, 128)] = z[t]
    total = None
    for d in range(5):
        term = product(u_ref[:, d * 256 : d * 256 + 256], gather_ref[d * 256 : d * 256 + 256, :])
        total = term if total is None else total + term
    own, beside = total[:, :128].reshape(16, 8, 128), total[:, 128:].reshape(16, 8, 128)
    head = iota((16, 8, 128), 2) < 64
    landed = own + jnp.where(head, pltpu.roll(beside, 1, 1), pltpu.roll(beside, 7, 1))
    for t in range(4):
        far_ref[t], far_ref[4 + t] = landed[t * 4], landed[t * 4 + 1]
        near_ref[t], near_ref[4 + t] = landed[t * 4 + 3], landed[t * 4 + 2]


def first_observe_kernel(far_ref, c0_ref, c1_ref, near_ref, *refs):
    observe([[ref[t] for ref in (far_ref, c0_ref, c1_ref, near_ref)] for t in range(4)], *order(refs))


def second_observe_kernel(*refs):
    rows = joined(*refs[:4])
    observe([[rows[q][t] for q in range(4)] for t in range(4)], *order(refs[4:]))


def order(refs):
    *fields, far_ref, near_ref, u_ref = refs
    return *fields, u_ref, far_ref, near_ref


def joined(far_ref, near_ref, from_far_ref, from_near_ref):
    rows = [None] * 4
    for mine, theirs, halo, own in ((far_ref, from_far_ref, 0, 1), (near_ref, from_near_ref, 3, 2)):
        rows[halo] = [mine[t] + theirs[4 + t] for t in range(4)]
        rows[own] = [mine[4 + t] + theirs[t] for t in range(4)]
    return rows


def adjoint_rows(place_ref, refs):
    rows = joined(*refs)
    rows[0] = [if_inside(place_ref, x) for x in rows[0]]
    return rows


def smoothed_back(e_refs, rows, s_ref):
    def body(b, carry):
        back = []
        for q in range(4):
            x = e_refs[q][pl.ds(b * 16, 16)].reshape(4, 4, 8, 128)
            total = x[:, 0] * rows[q][0]
            for t in range(1, 4):
                total = total + x[:, t] * rows[q][t]
            back.append(total)
        for r in range(2):
            s_ref[r, pl.ds(b * 4, 4)] = C_MID * back[r + 1] + C_SIDE * (back[r] + back[r + 2])
        return carry

    lax.fori_loop(0, 8, body, 0, unroll=2)


def middle_kernel(
    widths_ref, place_ref, lf_ref, ln_ref, rf_ref, rn_ref, ef_ref, e0_ref, e1_ref, en_ref,
    band_ref, v_ref, new_ref, part_ref, s_ref,
):
    rows = adjoint_rows(place_ref, (lf_ref, ln_ref, rf_ref, rn_ref))
    e_refs = (ef_ref, e0_ref, e1_ref, en_ref)
    smoothed_back(e_refs, rows, s_ref)
    for r in range(2):
        scale = scale_of(width_of(widths_ref, place_ref, r))
        for b in range(2):
            at = pl.ds(b * 16, 16)
            old = v_ref[r, at]
            gradient = old + filtered(s_ref[r, at], band_ref[r], scale)
            new = old - STEP_SIZE * gradient
            new_ref[r, at] = new
            s_ref[r, at] = filtered(new, band_ref[r], scale)

    def body(b, sums):
        sums = list(sums)
        for i in range(4):
            m = b * 4 + i
            w = [s_ref[r, m] for r in range(2)]
            forward = [
                C_SIDE * w[0],
                C_MID * w[0] + C_SIDE * w[1],
                C_MID * w[1] + C_SIDE * w[0],
                C_SIDE * w[1],
            ]
            for q in range(4):
                for t in range(4):
                    sums[q * 4 + t] = sums[q * 4 + t] + e_refs[q][m * 4 + t] * forward[q]
        return tuple(sums)

    sums = list(lax.fori_loop(0, 8, body, (jnp.zeros((8, 128), F32),) * 16))
    for t in range(4):
        part_ref[t], part_ref[4 + t] = if_inside(place_ref, sums[t]), sums[4 + t]
        part_ref[8 + t], part_ref[12 + t] = sums[12 + t], sums[8 + t]


def last_kernel(
    widths_ref, place_ref, lf_ref, ln_ref, rf_ref, rn_ref, ef_ref, e0_ref, e1_ref, en_ref,
    band_ref, v_ref, out_ref, s_ref,
):
    rows = adjoint_rows(place_ref, (lf_ref, ln_ref, rf_ref, rn_ref))
    smoothed_back((ef_ref, e0_ref, e1_ref, en_ref), rows, s_ref)
    for r in range(2):
        scale = scale_of(width_of(widths_ref, place_ref, r))
        for b in range(2):
            at = pl.ds(b * 16, 16)
            old = v_ref[r, at]
            gradient = old + filtered(s_ref[r, at], band_ref[r], scale)
            s_ref[r, at] = old - STEP_SIZE * gradient
    for b in range(2):
        at = pl.ds(b * 16, 16)
        out_ref[at, pl.ds(0, 8, stride=2), :] = if_odd(place_ref, s_ref[1, at], s_ref[0, at])
        out_ref[at, pl.ds(1, 8, stride=2), :] = if_odd(place_ref, s_ref[0, at], s_ref[1, at])


def swapped(far, near):
    bands = lax.axis_size("lat")
    ends = (0, bands - 1)
    pairs = [(i, i if i in ends else i + (1 if i % 2 else -1)) for i in range(bands)]
    far = lax.ppermute(far, "lat", pairs)
    near = lax.ppermute(near, "lat", [(i, i ^ 1) for i in range(bands)])
    return far, near


def tiles(x):
    (rows, cols) = x.shape[-2:]
    x = x.reshape(-1, rows, cols // 128, 128).transpose(0, 2, 1, 3)
    return x.reshape(-1, cols // 128 * rows, 128)


def descent(control, ensemble, widths, interp_source, interp_weight, obs_mask, innovation):
    v = tiles(control)
    e = tiles(ensemble)
    lat, last = lax.axis_index("lat"), lax.axis_size("lat") - 1
    place = jnp.stack([lat % 2, (lat != 0) & (lat != last)]).astype(jnp.int32)
    scalars = (widths, place)
    row, rows = shape(32, 8, 128), shape(2, 32, 8, 128)
    band = jax.ShapeDtypeStruct((2, 256, 128), jnp.bfloat16)
    w0, w1, old, band = call(filter_kernel, (row, row, rows, band), (v,), scalars)
    far, near = swapped(w0, w1)
    e, w0, w1 = lax.optimization_barrier((e, w0, w1))
    e0, e1 = call(split_kernel, (shape(128, 8, 128),) * 2, (e,), (place,))
    e_far, e_near = swapped(e0, e1)
    fields = call(
        planes_kernel,
        (
            shape(15, 8, 8, 128),
            shape(4, 8, 8, 128),
            shape(4, 8, 8, 128),
            jax.ShapeDtypeStruct((256, 1280), jnp.bfloat16),
            jax.ShapeDtypeStruct((1280, 256), jnp.bfloat16),
        ),
        tuple(tiles(x) for x in (interp_source, interp_weight, obs_mask, innovation)),
        (place,),
    )
    part = call(first_kernel, shape(8, 8, 128), (w0, w1, far, near, e0, e1), (place,))
    four, eight = shape(4, 8, 128), shape(8, 8, 128)
    c0, c1 = call(sum_kernel, (four, four), (lax.all_gather(part, "mem"),))
    far, near = swapped(c0, c1)
    refined = ((128, 1280),)
    sent = call(
        first_observe_kernel, (eight, eight), (far, c0, c1, near) + tuple(fields), scratch=refined
    )
    ensembles = (e_far, e0, e1, e_near, band)
    smoothed = ((2, 32, 8, 128),)
    new, part = call(
        middle_kernel,
        (rows, shape(16, 8, 128)),
        tuple(sent) + swapped(*sent) + ensembles + (old,),
        scalars,
        smoothed,
    )
    sent = call(sum_kernel, (eight, eight), (lax.all_gather(part, "mem"),))
    sent = call(
        second_observe_kernel,
        (eight, eight),
        tuple(sent) + swapped(*sent) + tuple(fields),
        scratch=refined,
    )
    out = call(
        last_kernel,
        shape(32, 16, 128),
        tuple(sent) + swapped(*sent) + ensembles + (new,),
        scalars,
        smoothed,
    )
    return out.reshape(32, 8, 2, 128).transpose(0, 2, 1, 3).reshape(control.shape)


def solution(mesh):
    in_specs = (
        P("mem", "lat", None),
        P("mem", None, "lat", None),
        P("lat"),
        P(None, "lat", None),
        P(None, "lat", None),
        P(None, "lat", None),
        P(None, "lat", None),
    )
    out_specs = P("mem", "lat", None)
    return jax.shard_map(descent, mesh=mesh, in_specs=in_specs, out_specs=out_specs, check_vma=False)
```

```python
import jax
import jax.numpy as jnp
import numpy as np
from jax import lax
from jax.experimental import pallas as pl
from jax.experimental.pallas import tpu as pltpu
from jax.sharding import PartitionSpec as P

STEP_SIZE = 0.5
C_MID = 0.5
C_SIDE = 0.25

F32 = jnp.float32
LIMIT = 40 * 1024 * 1024


def shape(*dims):
    return jax.ShapeDtypeStruct(dims, F32)


def call(kernel, outs, args, scalars=(), scratch=(), flops=1_000_000):
    in_specs = [pl.BlockSpec(memory_space=pltpu.SMEM)] * len(scalars)
    in_specs += [pl.BlockSpec(memory_space=pltpu.VMEM)] * len(args)
    args = tuple(scalars) + tuple(args)
    return pl.pallas_call(
        kernel,
        out_shape=outs,
        in_specs=in_specs,
        out_specs=jax.tree.map(lambda _: pl.BlockSpec(memory_space=pltpu.VMEM), outs),
        scratch_shapes=[pltpu.VMEM(dims, F32) for dims in scratch],
        compiler_params=pltpu.CompilerParams(vmem_limit_bytes=LIMIT),
        cost_estimate=pl.CostEstimate(flops=flops, transcendentals=0, bytes_accessed=1_000_000),
    )(*args)


def iota(shape_, dim):
    return lax.broadcasted_iota(jnp.int32, shape_, dim)


def position(k):
    return jnp.where(k < 128, k, jnp.where(k < 192, k, k - 256))


def refining_matrix():
    k = np.arange(256)
    place = np.where(k < 128, k, np.where(k < 192, k, k - 256))
    n, lane = np.arange(1280) // 128, np.arange(1280) % 128
    source = n % 2 * 64 + lane // 2 + n // 2 - 2
    return jnp.asarray(place[:, None] == source[None, :], jnp.bfloat16)


def widened(x):
    n = x.shape[0]
    y = jnp.where(iota(x.shape, 2) < 64, pltpu.roll(x, 7, 1), pltpu.roll(x, 1, 1))
    return jnp.concatenate([x.reshape(n * 8, 128), y.reshape(n * 8, 128)], axis=1)


def product(x, matrix):
    high = x.astype(jnp.bfloat16)
    rest = x - high.astype(F32)
    middle = rest.astype(jnp.bfloat16)
    low = (rest - middle.astype(F32)).astype(jnp.bfloat16)
    total = jnp.dot(low, matrix, preferred_element_type=F32)
    total = total + jnp.dot(middle, matrix, preferred_element_type=F32)
    return total + jnp.dot(high, matrix, preferred_element_type=F32)


def filtered(x, band, scale):
    return product(widened(x), band).reshape(x.shape) * scale


def scale_of(width):
    return 1.0 / (2.0 * jnp.full((8, 128), width, jnp.int32).astype(F32) + 1.0)


def if_inside(place_ref, x):
    return jnp.where(jnp.full((8, 128), place_ref[1], jnp.int32) > 0, x, 0.0)


def if_odd(place_ref, odd, even):
    return jnp.where(jnp.full((8, 128), place_ref[0], jnp.int32) > 0, odd, even)


def filter_kernel(place_ref, v_ref, w0_ref, w1_ref, old_ref, band_ref):
    away = jnp.abs(position(iota((256, 128), 0)) - iota((256, 128), 1))
    for r, out in ((0, w0_ref), (1, w1_ref)):
        width = place_ref[2 + r]
        inside = away <= jnp.full((256, 128), width, jnp.int32)
        band = jnp.where(inside, 1.0, 0.0).astype(jnp.bfloat16)
        band_ref[r] = band
        for b in range(2):
            at = pl.ds(b * 16, 16)
            top, bottom = (v_ref[at, pl.ds(n, 8, stride=2), :] for n in range(2))
            x = if_odd(place_ref, top, bottom) if r else if_odd(place_ref, bottom, top)
            old_ref[r, at] = x
            out[at] = filtered(x, band, scale_of(width))


def split_kernel(place_ref, e_ref, *out_refs):
    for half in range(2):

        def body(b, carry, half=half):
            at = pl.ds(half * 64 + b * 8, 8)
            top, bottom = (e_ref[at, pl.ds(n, 8, stride=2), :] for n in range(2))
            out_refs[half][pl.ds(b * 8, 8)] = if_odd(place_ref, bottom, top)
            out_refs[2 + half][pl.ds(b * 8, 8)] = if_odd(place_ref, top, bottom)
            return carry

        lax.fori_loop(0, 8, body, 0)


def planes_kernel(place_ref, src_ref, wgt_ref, msk_ref, inn_ref, planes_ref, mask_ref, target_ref):
    parent = iota((8, 128), 0) * 128 + iota((8, 128), 1) // 2
    odd = jnp.full((8, 128), place_ref[0], jnp.int32)
    for j in range(8):
        half, fr = j // 4, j % 4
        at, mirrored = pl.ds(j, 8, stride=8), pl.ds(half * 4 + 3 - fr, 8, stride=8)

        def row(ref, n, at=at, mirrored=mirrored):
            return jnp.where(odd > 0, ref[n, mirrored, :], ref[n, at, :])

        own_row = jnp.where(odd > 0, 1 - fr // 2, fr // 2)
        codes, weights = [], []
        for s in range(4):
            src = row(src_ref, s)
            row_shift = lax.shift_right_logical(src, 10) - (own_row + 1)
            row_shift = jnp.where(odd > 0, -row_shift, row_shift)
            col = jnp.bitwise_and(src, 1023)
            col_shift = jnp.bitwise_and(col - parent - half * 64 + 2, 1023) - 2
            codes.append((row_shift + 1) * 5 + col_shift + 2)
            weights.append(row(wgt_ref, s))
        for n in range(15):
            total = jnp.where(codes[0] == n, weights[0], 0.0)
            for s in range(1, 4):
                total = total + jnp.where(codes[s] == n, weights[s], 0.0)
            planes_ref[n, j] = total
        for t in range(4):
            mask_ref[t, j] = row(msk_ref, t).astype(F32)
            target_ref[t, j] = row(inn_ref, t)


def first_kernel(place_ref, w0_ref, w1_ref, far_ref, near_ref, *refs):
    *e_refs, part_ref = refs
    sums = (jnp.zeros((8, 128), F32),) * 8
    for half in range(2):

        def body(n, sums, half=half):
            m = half * 16 + n
            a, b = w0_ref[m], w1_ref[m]
            f0 = C_MID * a + C_SIDE * (if_inside(place_ref, far_ref[m]) + b)
            f1 = C_MID * b + C_SIDE * (a + near_ref[m])
            sums = list(sums)
            for t in range(4):
                sums[t] = sums[t] + e_refs[half][n * 4 + t] * f0
                sums[4 + t] = sums[4 + t] + e_refs[2 + half][n * 4 + t] * f1
            return tuple(sums)

        sums = lax.fori_loop(0, 16, body, sums, unroll=4)
    for n in range(8):
        part_ref[n] = sums[n]


def sum_kernel(parts_ref, a_ref, b_ref):
    count = a_ref.shape[0]
    for n in range(2 * count):
        total = (parts_ref[0, n] + parts_ref[1, n]) + (parts_ref[2, n] + parts_ref[3, n])
        if n < count:
            a_ref[n] = total
        else:
            b_ref[n - count] = total


def stencil(a, b):
    lane = iota((8, 128), 1)
    a1, b1 = pltpu.roll(a, 1, 1), pltpu.roll(b, 1, 1)
    left_a = jnp.where(lane == 0, pltpu.roll(b1, 1, 0), a1)
    left_b = jnp.where(lane == 0, a1, b1)
    a2, b2 = pltpu.roll(a, 127, 1), pltpu.roll(b, 127, 1)
    right_a = jnp.where(lane == 127, b2, a2)
    right_b = jnp.where(lane == 127, pltpu.roll(a2, 7, 0), b2)
    return 0.5 * a + 0.25 * (left_a + right_a), 0.5 * b + 0.25 * (left_b + right_b)


def observe(rows, planes_ref, mask_ref, target_ref, refine_ref, gather_ref, u_ref, far_ref, near_ref):
    window = jnp.stack([rows[t][q] for t in range(4) for q in range(4)])
    u_ref[...] = product(widened(window), refine_ref[...])

    def piece(t, q, d, half):
        n = d * 2 + half
        return u_ref[pl.ds((t * 4 + q) * 8, 8), pl.ds(n * 128, 128)]

    back = {}
    for r in range(2):
        fine = {}
        for half in range(2):
            for rs in range(-1, 2):
                for d in range(5):
                    u = [piece(t, r + 1 + rs, d, half) for t in range(4)]
                    for fr in (2 * r, 2 * r + 1):
                        plane = planes_ref[(rs + 1) * 5 + d, half * 4 + fr]
                        for t in range(4):
                            key = (t, fr, half)
                            fine[key] = fine[key] + plane * u[t] if key in fine else plane * u[t]
        for t in range(4):
            for fr in (2 * r, 2 * r + 1):
                pair = stencil(fine[t, fr, 0], fine[t, fr, 1])
                pair = [
                    mask_ref[t, half * 4 + fr] * (pair[half] - target_ref[t, half * 4 + fr])
                    for half in range(2)
                ]
                back[t, fr, 0], back[t, fr, 1] = stencil(*pair)
    for half in range(2):
        for d in range(5):
            n = d * 2 + half
            for q in range(4):
                z = [None] * 4
                for fr in range(4):
                    rs = q - 1 - fr // 2
                    if -1 <= rs <= 1:
                        plane = planes_ref[(rs + 1) * 5 + d, half * 4 + fr]
                        for t in range(4):
                            term = plane * back[t, fr, half]
                            z[t] = term if z[t] is None else z[t] + term
                for t in range(4):
                    u_ref[pl.ds((t * 4 + q) * 8, 8), pl.ds(n * 128, 128)] = z[t]
    total = None
    for d in range(5):
        term = product(u_ref[:, d * 256 : d * 256 + 256], gather_ref[d * 256 : d * 256 + 256, :])
        total = term if total is None else total + term
    own, beside = total[:, :128].reshape(16, 8, 128), total[:, 128:].reshape(16, 8, 128)
    head = iota((16, 8, 128), 2) < 64
    landed = own + jnp.where(head, pltpu.roll(beside, 1, 1), pltpu.roll(beside, 7, 1))
    for t in range(4):
        far_ref[t], far_ref[4 + t] = landed[t * 4], landed[t * 4 + 1]
        near_ref[t], near_ref[4 + t] = landed[t * 4 + 3], landed[t * 4 + 2]


def first_observe_kernel(far_ref, c0_ref, c1_ref, near_ref, *refs):
    observe([[ref[t] for ref in (far_ref, c0_ref, c1_ref, near_ref)] for t in range(4)], *order(refs))


def second_observe_kernel(*refs):
    rows = joined(*refs[:4])
    observe([[rows[q][t] for q in range(4)] for t in range(4)], *order(refs[4:]))


def order(refs):
    *fields, far_ref, near_ref, u_ref = refs
    return *fields, u_ref, far_ref, near_ref


def joined(far_ref, near_ref, from_far_ref, from_near_ref):
    rows = [None] * 4
    for mine, theirs, halo, own in ((far_ref, from_far_ref, 0, 1), (near_ref, from_near_ref, 3, 2)):
        rows[halo] = [mine[t] + theirs[4 + t] for t in range(4)]
        rows[own] = [mine[4 + t] + theirs[t] for t in range(4)]
    return rows


def adjoint_rows(place_ref, refs):
    rows = joined(*refs)
    rows[0] = [if_inside(place_ref, x) for x in rows[0]]
    return rows


def smoothed_back(e_refs, rows, s_ref):
    for half in range(2):

        def body(b, carry, half=half):
            back = []
            for q in range(4):
                x = e_refs[q * 2 + half][pl.ds(b * 16, 16)].reshape(4, 4, 8, 128)
                total = x[:, 0] * rows[q][0]
                for t in range(1, 4):
                    total = total + x[:, t] * rows[q][t]
                back.append(total)
            at = pl.ds(half * 16 + b * 4, 4)
            for r in range(2):
                s_ref[r, at] = C_MID * back[r + 1] + C_SIDE * (back[r] + back[r + 2])
            return carry

        lax.fori_loop(0, 4, body, 0, unroll=2)


def middle_kernel(place_ref, lf_ref, ln_ref, rf_ref, rn_ref, *refs):
    *e_refs, band_ref, v_ref, new_ref, part_ref, s_ref = refs
    rows = adjoint_rows(place_ref, (lf_ref, ln_ref, rf_ref, rn_ref))
    smoothed_back(e_refs, rows, s_ref)
    for r in range(2):
        scale = scale_of(place_ref[2 + r])
        for b in range(2):
            at = pl.ds(b * 16, 16)
            old = v_ref[r, at]
            gradient = old + filtered(s_ref[r, at], band_ref[r], scale)
            new = old - STEP_SIZE * gradient
            new_ref[r, at] = new
            s_ref[r, at] = filtered(new, band_ref[r], scale)
    sums = (jnp.zeros((8, 128), F32),) * 16
    for half in range(2):

        def body(b, sums, half=half):
            sums = list(sums)
            for i in range(4):
                n = b * 4 + i
                w = [s_ref[r, half * 16 + n] for r in range(2)]
                forward = [
                    C_SIDE * w[0],
                    C_MID * w[0] + C_SIDE * w[1],
                    C_MID * w[1] + C_SIDE * w[0],
                    C_SIDE * w[1],
                ]
                for q in range(4):
                    for t in range(4):
                        x = e_refs[q * 2 + half][n * 4 + t]
                        sums[q * 4 + t] = sums[q * 4 + t] + x * forward[q]
            return tuple(sums)

        sums = lax.fori_loop(0, 4, body, sums)
    for t in range(4):
        part_ref[t], part_ref[4 + t] = if_inside(place_ref, sums[t]), sums[4 + t]
        part_ref[8 + t], part_ref[12 + t] = sums[12 + t], sums[8 + t]


def last_kernel(place_ref, lf_ref, ln_ref, rf_ref, rn_ref, *refs):
    *e_refs, band_ref, v_ref, out_ref, s_ref = refs
    rows = adjoint_rows(place_ref, (lf_ref, ln_ref, rf_ref, rn_ref))
    smoothed_back(e_refs, rows, s_ref)
    for r in range(2):
        scale = scale_of(place_ref[2 + r])
        for b in range(2):
            at = pl.ds(b * 16, 16)
            old = v_ref[r, at]
            gradient = old + filtered(s_ref[r, at], band_ref[r], scale)
            s_ref[r, at] = old - STEP_SIZE * gradient
    for b in range(2):
        at = pl.ds(b * 16, 16)
        out_ref[at, pl.ds(0, 8, stride=2), :] = if_odd(place_ref, s_ref[1, at], s_ref[0, at])
        out_ref[at, pl.ds(1, 8, stride=2), :] = if_odd(place_ref, s_ref[0, at], s_ref[1, at])


def from_far(x):
    bands = lax.axis_size("lat")
    pairs = [(i, i if i in (0, bands - 1) else i + (1 if i % 2 else -1)) for i in range(bands)]
    return lax.ppermute(x, "lat", pairs)


def from_near(x):
    return lax.ppermute(x, "lat", [(i, i ^ 1) for i in range(lax.axis_size("lat"))])


def swapped(far, near):
    return from_far(far), from_near(near)


def tiles(x):
    (rows, cols) = x.shape[-2:]
    x = x.reshape(-1, rows, cols // 128, 128).transpose(0, 2, 1, 3)
    return x.reshape(-1, cols // 128 * rows, 128)


def descent(control, ensemble, widths, interp_source, interp_weight, obs_mask, innovation):
    v = tiles(control)
    e = tiles(ensemble)
    lat, last = lax.axis_index("lat"), lax.axis_size("lat") - 1
    odd = lat % 2
    ends = jnp.stack([odd, (lat != 0) & (lat != last)]).astype(jnp.int32)
    place = jnp.concatenate([ends, jnp.where(odd > 0, widths[::-1], widths)])
    scalars = (place,)
    row, rows = shape(32, 8, 128), shape(2, 32, 8, 128)
    band = jax.ShapeDtypeStruct((2, 256, 128), jnp.bfloat16)
    w0, w1, old, band = call(filter_kernel, (row, row, rows, band), (v,), scalars)
    far, near = swapped(w0, w1)
    e0, e0_late, e1, e1_late = call(split_kernel, (shape(64, 8, 128),) * 4, (e,), scalars)
    ensembles = (
        *(from_far(e0), from_far(e0_late)),
        *(e0, e0_late, e1, e1_late),
        *(from_near(e1), from_near(e1_late)),
        band,
    )
    fields = call(
        planes_kernel,
        (shape(15, 8, 8, 128), shape(4, 8, 8, 128), shape(4, 8, 8, 128)),
        tuple(tiles(x) for x in (interp_source, interp_weight, obs_mask, innovation)),
        scalars,
    )
    refine = refining_matrix()
    fields = tuple(fields) + (refine, refine.T)
    part = call(
        first_kernel, shape(8, 8, 128), (w0, w1, far, near, e0, e0_late, e1, e1_late), scalars
    )
    four, eight = shape(4, 8, 128), shape(8, 8, 128)
    c0, c1 = call(sum_kernel, (four, four), (lax.all_gather(part, "mem"),))
    far, near = swapped(c0, c1)
    refined = ((128, 1280),)
    sent = call(
        first_observe_kernel, (eight, eight), (far, c0, c1, near) + fields, scratch=refined
    )
    smoothed = ((2, 32, 8, 128),)
    new, part = call(
        middle_kernel,
        (rows, shape(16, 8, 128)),
        tuple(sent) + swapped(*sent) + ensembles + (old,),
        scalars,
        smoothed,
    )
    sent = call(sum_kernel, (eight, eight), (lax.all_gather(part, "mem"),))
    sent = call(
        second_observe_kernel,
        (eight, eight),
        tuple(sent) + swapped(*sent) + fields,
        scratch=refined,
    )
    out = call(
        last_kernel,
        shape(32, 16, 128),
        tuple(sent) + swapped(*sent) + ensembles + (new,),
        scalars,
        smoothed,
    )
    return out.reshape(32, 8, 2, 128).transpose(0, 2, 1, 3).reshape(control.shape)


def solution(mesh):
    in_specs = (
        P("mem", "lat", None),
        P("mem", None, "lat", None),
        P("lat"),
        P(None, "lat", None),
        P(None, "lat", None),
        P(None, "lat", None),
        P(None, "lat", None),
    )
    out_specs = P("mem", "lat", None)
    return jax.shard_map(descent, mesh=mesh, in_specs=in_specs, out_specs=out_specs, check_vma=False)
```

```python
import jax
import jax.numpy as jnp
import numpy as np
from jax import lax
from jax.experimental import pallas as pl
from jax.experimental.pallas import tpu as pltpu
from jax.sharding import PartitionSpec as P

STEP_SIZE = 0.5
C_MID = 0.5
C_SIDE = 0.25

F32 = jnp.float32
LIMIT = 40 * 1024 * 1024


def shape(*dims):
    return jax.ShapeDtypeStruct(dims, F32)


def call(kernel, outs, args, scalars=(), scratch=(), far_args=()):
    in_specs = [pl.BlockSpec(memory_space=pltpu.SMEM)] * len(scalars)
    in_specs += [pl.BlockSpec(memory_space=pltpu.HBM)] * len(far_args)
    in_specs += [pl.BlockSpec(memory_space=pltpu.VMEM)] * len(args)
    far_args = tuple(pltpu.with_memory_space_constraint(x, pltpu.HBM) for x in far_args)
    args = tuple(scalars) + far_args + tuple(args)
    return pl.pallas_call(
        kernel,
        out_shape=outs,
        in_specs=in_specs,
        out_specs=jax.tree.map(lambda _: pl.BlockSpec(memory_space=pltpu.VMEM), outs),
        scratch_shapes=list(scratch),
        compiler_params=pltpu.CompilerParams(vmem_limit_bytes=LIMIT),
        cost_estimate=pl.CostEstimate(flops=1_000_000, transcendentals=0, bytes_accessed=1_000_000),
    )(*args)


def iota(shape_, dim):
    return lax.broadcasted_iota(jnp.int32, shape_, dim)


def position(k):
    return jnp.where(k < 128, k, jnp.where(k < 192, k, k - 256))


def refining_matrix():
    k = np.arange(256)
    place = np.where(k < 128, k, np.where(k < 192, k, k - 256))
    n, lane = np.arange(1280) // 128, np.arange(1280) % 128
    source = n % 2 * 64 + lane // 2 + n // 2 - 2
    return jnp.asarray(place[:, None] == source[None, :], jnp.bfloat16)


def widened(x):
    n = x.shape[0]
    y = jnp.where(iota(x.shape, 2) < 64, pltpu.roll(x, 7, 1), pltpu.roll(x, 1, 1))
    return jnp.concatenate([x.reshape(n * 8, 128), y.reshape(n * 8, 128)], axis=1)


def product(x, matrix):
    high = x.astype(jnp.bfloat16)
    rest = x - high.astype(F32)
    middle = rest.astype(jnp.bfloat16)
    low = (rest - middle.astype(F32)).astype(jnp.bfloat16)
    total = jnp.dot(low, matrix, preferred_element_type=F32)
    total = total + jnp.dot(middle, matrix, preferred_element_type=F32)
    return total + jnp.dot(high, matrix, preferred_element_type=F32)


def filtered(x, band, scale):
    return product(widened(x), band).reshape(x.shape) * scale


def scale_of(width):
    return 1.0 / (2.0 * jnp.full((8, 128), width, jnp.int32).astype(F32) + 1.0)


def if_inside(place_ref, x):
    return jnp.where(jnp.full((8, 128), place_ref[1], jnp.int32) > 0, x, 0.0)


def if_odd(place_ref, odd, even):
    return jnp.where(jnp.full((8, 128), place_ref[0], jnp.int32) > 0, odd, even)


def filter_kernel(
    place_ref, widths_hbm, v_hbm, w0_ref, w1_ref, old_ref, band_ref, widths_ref, v_ref, sems
):
    fetch = [pltpu.make_async_copy(widths_hbm, widths_ref, sems.at[0])]
    for b in range(2):
        at = pl.ds(b * 16, 16)
        fetch.append(pltpu.make_async_copy(v_hbm.at[at], v_ref.at[at], sems.at[1 + b]))
    for copy in fetch:
        copy.start()
    away = jnp.abs(position(iota((256, 128), 0)) - iota((256, 128), 1))
    fetch[0].wait()
    scales = []
    for r in range(2):
        width = widths_ref[r + place_ref[0] * (1 - 2 * r)]
        inside = away <= jnp.full((256, 128), width, jnp.int32)
        band_ref[r] = jnp.where(inside, 1.0, 0.0).astype(jnp.bfloat16)
        scales.append(scale_of(width))
    for b in range(2):
        at = pl.ds(b * 16, 16)
        fetch[1 + b].wait()
        top, bottom = (v_ref[at, pl.ds(n, 8, stride=2), :] for n in range(2))
        for r, out in ((0, w0_ref), (1, w1_ref)):
            x = if_odd(place_ref, top, bottom) if r else if_odd(place_ref, bottom, top)
            old_ref[r, at] = x
            out[at] = filtered(x, band_ref[r], scales[r])


def split_kernel(place_ref, e_hbm, far_ref, far_late_ref, near_ref, e_ref, sems):
    fetch = []
    for part in range(4):
        at = pl.ds(part * 32, 32)
        fetch.append(pltpu.make_async_copy(e_hbm.at[at], e_ref.at[at], sems.at[part]))
        fetch[-1].start()
    for part in range(4):
        fetch[part].wait()
        out = (far_ref, far_late_ref)[part // 2]

        def body(b, carry, part=part, out=out):
            at = pl.ds(part * 32 + b * 8, 8)
            top, bottom = (e_ref[at, pl.ds(n, 8, stride=2), :] for n in range(2))
            out[pl.ds(part % 2 * 32 + b * 8, 8)] = if_odd(place_ref, bottom, top)
            near_ref[at] = if_odd(place_ref, top, bottom)
            return carry

        lax.fori_loop(0, 4, body, 0)


def planes_kernel(place_ref, src_ref, wgt_ref, msk_ref, inn_ref, planes_ref, mask_ref, target_ref):
    parent = iota((8, 128), 0) * 128 + iota((8, 128), 1) // 2
    odd = jnp.full((8, 128), place_ref[0], jnp.int32)
    for j in range(8):
        half, fr = j // 4, j % 4
        at, mirrored = pl.ds(j, 8, stride=8), pl.ds(half * 4 + 3 - fr, 8, stride=8)

        def row(ref, n, at=at, mirrored=mirrored):
            return jnp.where(odd > 0, ref[n, mirrored, :], ref[n, at, :])

        own_row = jnp.where(odd > 0, 1 - fr // 2, fr // 2)
        codes, weights = [], []
        for s in range(4):
            src = row(src_ref, s)
            row_shift = lax.shift_right_logical(src, 10) - (own_row + 1)
            row_shift = jnp.where(odd > 0, -row_shift, row_shift)
            col = jnp.bitwise_and(src, 1023)
            col_shift = jnp.bitwise_and(col - parent - half * 64 + 2, 1023) - 2
            codes.append((row_shift + 1) * 5 + col_shift + 2)
            weights.append(row(wgt_ref, s))
        for n in range(15):
            total = jnp.where(codes[0] == n, weights[0], 0.0)
            for s in range(1, 4):
                total = total + jnp.where(codes[s] == n, weights[s], 0.0)
            planes_ref[n, j] = total
        for t in range(4):
            mask_ref[t, j] = row(msk_ref, t).astype(F32)
            target_ref[t, j] = row(inn_ref, t)


def members(e_refs, q, half):
    if q < 2:
        return e_refs[q * 2 + half], 0
    return e_refs[q + 2], half * 64


def first_kernel(place_ref, w0_ref, w1_ref, far_ref, near_ref, *refs):
    *e_refs, part_ref = refs
    sums = (jnp.zeros((8, 128), F32),) * 8
    for half in range(2):

        def body(n, sums, half=half):
            m = half * 16 + n
            a, b = w0_ref[m], w1_ref[m]
            f0 = C_MID * a + C_SIDE * (if_inside(place_ref, far_ref[m]) + b)
            f1 = C_MID * b + C_SIDE * (a + near_ref[m])
            sums = list(sums)
            for t in range(4):
                sums[t] = sums[t] + e_refs[half][n * 4 + t] * f0
                sums[4 + t] = sums[4 + t] + e_refs[2][half * 64 + n * 4 + t] * f1
            return tuple(sums)

        sums = lax.fori_loop(0, 16, body, sums, unroll=4)
    for n in range(8):
        part_ref[n] = sums[n]


def sum_kernel(parts_ref, a_ref, b_ref):
    count = a_ref.shape[0]
    for n in range(2 * count):
        total = (parts_ref[0, n] + parts_ref[1, n]) + (parts_ref[2, n] + parts_ref[3, n])
        if n < count:
            a_ref[n] = total
        else:
            b_ref[n - count] = total


def stencil(a, b):
    lane = iota((8, 128), 1)
    a1, b1 = pltpu.roll(a, 1, 1), pltpu.roll(b, 1, 1)
    left_a = jnp.where(lane == 0, pltpu.roll(b1, 1, 0), a1)
    left_b = jnp.where(lane == 0, a1, b1)
    a2, b2 = pltpu.roll(a, 127, 1), pltpu.roll(b, 127, 1)
    right_a = jnp.where(lane == 127, b2, a2)
    right_b = jnp.where(lane == 127, pltpu.roll(a2, 7, 0), b2)
    return 0.5 * a + 0.25 * (left_a + right_a), 0.5 * b + 0.25 * (left_b + right_b)


def observe(rows, planes_ref, mask_ref, target_ref, refine_ref, gather_ref, u_ref, far_ref, near_ref):
    window = jnp.stack([rows[t][q] for t in range(4) for q in range(4)])
    u_ref[...] = product(widened(window), refine_ref[...])

    def piece(t, q, d, half):
        n = d * 2 + half
        return u_ref[pl.ds((t * 4 + q) * 8, 8), pl.ds(n * 128, 128)]

    back = {}
    for r in range(2):
        fine = {}
        for half in range(2):
            for rs in range(-1, 2):
                for d in range(5):
                    u = [piece(t, r + 1 + rs, d, half) for t in range(4)]
                    for fr in (2 * r, 2 * r + 1):
                        plane = planes_ref[(rs + 1) * 5 + d, half * 4 + fr]
                        for t in range(4):
                            key = (t, fr, half)
                            fine[key] = fine[key] + plane * u[t] if key in fine else plane * u[t]
        for t in range(4):
            for fr in (2 * r, 2 * r + 1):
                pair = stencil(fine[t, fr, 0], fine[t, fr, 1])
                pair = [
                    mask_ref[t, half * 4 + fr] * (pair[half] - target_ref[t, half * 4 + fr])
                    for half in range(2)
                ]
                back[t, fr, 0], back[t, fr, 1] = stencil(*pair)
    for half in range(2):
        for d in range(5):
            n = d * 2 + half
            for q in range(4):
                z = [None] * 4
                for fr in range(4):
                    rs = q - 1 - fr // 2
                    if -1 <= rs <= 1:
                        plane = planes_ref[(rs + 1) * 5 + d, half * 4 + fr]
                        for t in range(4):
                            term = plane * back[t, fr, half]
                            z[t] = term if z[t] is None else z[t] + term
                for t in range(4):
                    u_ref[pl.ds((t * 4 + q) * 8, 8), pl.ds(n * 128, 128)] = z[t]
    total = None
    for d in range(5):
        term = product(u_ref[:, d * 256 : d * 256 + 256], gather_ref[d * 256 : d * 256 + 256, :])
        total = term if total is None else total + term
    own, beside = total[:, :128].reshape(16, 8, 128), total[:, 128:].reshape(16, 8, 128)
    head = iota((16, 8, 128), 2) < 64
    landed = own + jnp.where(head, pltpu.roll(beside, 1, 1), pltpu.roll(beside, 7, 1))
    for t in range(4):
        far_ref[t], far_ref[4 + t] = landed[t * 4], landed[t * 4 + 1]
        near_ref[t], near_ref[4 + t] = landed[t * 4 + 3], landed[t * 4 + 2]


def first_observe_kernel(far_ref, c0_ref, c1_ref, near_ref, *refs):
    observe([[ref[t] for ref in (far_ref, c0_ref, c1_ref, near_ref)] for t in range(4)], *order(refs))


def second_observe_kernel(*refs):
    rows = joined(*refs[:4])
    observe([[rows[q][t] for q in range(4)] for t in range(4)], *order(refs[4:]))


def order(refs):
    *fields, far_ref, near_ref, u_ref = refs
    return *fields, u_ref, far_ref, near_ref


def joined(far_ref, near_ref, from_far_ref, from_near_ref):
    rows = [None] * 4
    for mine, theirs, halo, own in ((far_ref, from_far_ref, 0, 1), (near_ref, from_near_ref, 3, 2)):
        rows[halo] = [mine[t] + theirs[4 + t] for t in range(4)]
        rows[own] = [mine[4 + t] + theirs[t] for t in range(4)]
    return rows


def adjoint_rows(place_ref, refs):
    rows = joined(*refs)
    rows[0] = [if_inside(place_ref, x) for x in rows[0]]
    return rows


def smoothed_back(e_refs, rows, s_ref):
    for half in range(2):

        def body(b, carry, half=half):
            back = []
            for q in range(4):
                ref, first = members(e_refs, q, half)
                x = ref[pl.ds(first + b * 16, 16)].reshape(4, 4, 8, 128)
                total = x[:, 0] * rows[q][0]
                for t in range(1, 4):
                    total = total + x[:, t] * rows[q][t]
                back.append(total)
            at = pl.ds(half * 16 + b * 4, 4)
            for r in range(2):
                s_ref[r, at] = C_MID * back[r + 1] + C_SIDE * (back[r] + back[r + 2])
            return carry

        lax.fori_loop(0, 4, body, 0, unroll=2)


def middle_kernel(place_ref, lf_ref, ln_ref, rf_ref, rn_ref, *refs):
    *e_refs, band_ref, v_ref, new_ref, part_ref, s_ref = refs
    rows = adjoint_rows(place_ref, (lf_ref, ln_ref, rf_ref, rn_ref))
    smoothed_back(e_refs, rows, s_ref)
    for r in range(2):
        scale = scale_of(place_ref[2 + r])
        for b in range(2):
            at = pl.ds(b * 16, 16)
            old = v_ref[r, at]
            gradient = old + filtered(s_ref[r, at], band_ref[r], scale)
            new = old - STEP_SIZE * gradient
            new_ref[r, at] = new
            s_ref[r, at] = filtered(new, band_ref[r], scale)
    sums = (jnp.zeros((8, 128), F32),) * 16
    for half in range(2):

        def body(b, sums, half=half):
            sums = list(sums)
            for i in range(4):
                n = b * 4 + i
                w = [s_ref[r, half * 16 + n] for r in range(2)]
                forward = [
                    C_SIDE * w[0],
                    C_MID * w[0] + C_SIDE * w[1],
                    C_MID * w[1] + C_SIDE * w[0],
                    C_SIDE * w[1],
                ]
                for q in range(4):
                    ref, first = members(e_refs, q, half)
                    for t in range(4):
                        x = ref[first + n * 4 + t]
                        sums[q * 4 + t] = sums[q * 4 + t] + x * forward[q]
            return tuple(sums)

        sums = lax.fori_loop(0, 4, body, sums)
    for t in range(4):
        part_ref[t], part_ref[4 + t] = if_inside(place_ref, sums[t]), sums[4 + t]
        part_ref[8 + t], part_ref[12 + t] = sums[12 + t], sums[8 + t]


def last_kernel(place_ref, lf_ref, ln_ref, rf_ref, rn_ref, *refs):
    *e_refs, band_ref, v_ref, out_ref, s_ref = refs
    rows = adjoint_rows(place_ref, (lf_ref, ln_ref, rf_ref, rn_ref))
    smoothed_back(e_refs, rows, s_ref)
    for r in range(2):
        scale = scale_of(place_ref[2 + r])
        for b in range(2):
            at = pl.ds(b * 16, 16)
            old = v_ref[r, at]
            gradient = old + filtered(s_ref[r, at], band_ref[r], scale)
            s_ref[r, at] = old - STEP_SIZE * gradient
    for b in range(2):
        at = pl.ds(b * 16, 16)
        out_ref[at, pl.ds(0, 8, stride=2), :] = if_odd(place_ref, s_ref[1, at], s_ref[0, at])
        out_ref[at, pl.ds(1, 8, stride=2), :] = if_odd(place_ref, s_ref[0, at], s_ref[1, at])


def from_far(x):
    bands = lax.axis_size("lat")
    pairs = [(i, i if i in (0, bands - 1) else i + (1 if i % 2 else -1)) for i in range(bands)]
    return lax.ppermute(x, "lat", pairs)


def from_near(x):
    return lax.ppermute(x, "lat", [(i, i ^ 1) for i in range(lax.axis_size("lat"))])


def swapped(far, near):
    return from_far(far), from_near(near)


def tiles(x):
    (rows, cols) = x.shape[-2:]
    x = x.reshape(-1, rows, cols // 128, 128).transpose(0, 2, 1, 3)
    return x.reshape(-1, cols // 128 * rows, 128)


def descent(control, ensemble, widths, interp_source, interp_weight, obs_mask, innovation):
    v = tiles(control)
    e = tiles(ensemble)
    lat, last = lax.axis_index("lat"), lax.axis_size("lat") - 1
    odd = lat % 2
    ends = jnp.stack([odd, (lat != 0) & (lat != last)]).astype(jnp.int32)
    place = jnp.concatenate([ends, jnp.where(odd > 0, widths[::-1], widths)])
    scalars = (place,)
    row, rows = shape(32, 8, 128), shape(2, 32, 8, 128)
    band = jax.ShapeDtypeStruct((2, 256, 128), jnp.bfloat16)
    w0, w1, old, band = call(
        filter_kernel,
        (row, row, rows, band),
        (),
        (ends,),
        (
            pltpu.SMEM((2,), jnp.int32),
            pltpu.VMEM((32, 16, 128), F32),
            pltpu.SemaphoreType.DMA((3,)),
        ),
        (widths, v),
    )
    far, near = swapped(w0, w1)
    e0, e0_late, e1 = call(
        split_kernel,
        (shape(64, 8, 128), shape(64, 8, 128), shape(128, 8, 128)),
        (),
        scalars,
        (pltpu.VMEM((128, 16, 128), F32), pltpu.SemaphoreType.DMA((4,))),
        (e,),
    )
    ensembles = (*(from_far(e0), from_far(e0_late)), *(e0, e0_late, e1, from_near(e1)), band)
    fields = call(
        planes_kernel,
        (shape(15, 8, 8, 128), shape(4, 8, 8, 128), shape(4, 8, 8, 128)),
        tuple(tiles(x) for x in (interp_source, interp_weight, obs_mask, innovation)),
        scalars,
    )
    refine = refining_matrix()
    fields = tuple(fields) + (refine, refine.T)
    part = call(
        first_kernel, shape(8, 8, 128), (w0, w1, far, near, e0, e0_late, e1), scalars
    )
    four, eight = shape(4, 8, 128), shape(8, 8, 128)
    c0, c1 = call(sum_kernel, (four, four), (lax.all_gather(part, "mem"),))
    far, near = swapped(c0, c1)
    refined = (pltpu.VMEM((128, 1280), F32),)
    sent = call(
        first_observe_kernel, (eight, eight), (far, c0, c1, near) + fields, scratch=refined
    )
    smoothed = (pltpu.VMEM((2, 32, 8, 128), F32),)
    new, part = call(
        middle_kernel,
        (rows, shape(16, 8, 128)),
        tuple(sent) + swapped(*sent) + ensembles + (old,),
        scalars,
        smoothed,
    )
    sent = call(sum_kernel, (eight, eight), (lax.all_gather(part, "mem"),))
    sent = call(
        second_observe_kernel,
        (eight, eight),
        tuple(sent) + swapped(*sent) + fields,
        scratch=refined,
    )
    out = call(
        last_kernel,
        shape(32, 16, 128),
        tuple(sent) + swapped(*sent) + ensembles + (new,),
        scalars,
        smoothed,
    )
    return out.reshape(32, 8, 2, 128).transpose(0, 2, 1, 3).reshape(control.shape)


def solution(mesh):
    in_specs = (
        P("mem", "lat", None),
        P("mem", None, "lat", None),
        P("lat"),
        P(None, "lat", None),
        P(None, "lat", None),
        P(None, "lat", None),
        P(None, "lat", None),
    )
    out_specs = P("mem", "lat", None)
    return jax.shard_map(descent, mesh=mesh, in_specs=in_specs, out_specs=out_specs, check_vma=False)
```

```python
import jax
import jax.numpy as jnp
import numpy as np
from jax import lax
from jax.experimental import pallas as pl
from jax.experimental.pallas import tpu as pltpu
from jax.sharding import PartitionSpec as P

STEP_SIZE = 0.5
C_MID = 0.5
C_SIDE = 0.25

F32 = jnp.float32
LIMIT = 40 * 1024 * 1024
PIECES = ((0, 8), (8, 24))


def shape(*dims):
    return jax.ShapeDtypeStruct(dims, F32)


def call(kernel, outs, args, scalars=(), scratch=(), far_args=()):
    in_specs = [pl.BlockSpec(memory_space=pltpu.SMEM)] * len(scalars)
    in_specs += [pl.BlockSpec(memory_space=pltpu.HBM)] * len(far_args)
    in_specs += [pl.BlockSpec(memory_space=pltpu.VMEM)] * len(args)
    far_args = tuple(pltpu.with_memory_space_constraint(x, pltpu.HBM) for x in far_args)
    args = tuple(scalars) + far_args + tuple(args)
    return pl.pallas_call(
        kernel,
        out_shape=outs,
        in_specs=in_specs,
        out_specs=jax.tree.map(lambda _: pl.BlockSpec(memory_space=pltpu.VMEM), outs),
        scratch_shapes=list(scratch),
        compiler_params=pltpu.CompilerParams(vmem_limit_bytes=LIMIT),
        cost_estimate=pl.CostEstimate(flops=1_000_000, transcendentals=0, bytes_accessed=1_000_000),
    )(*args)


def iota(shape_, dim):
    return lax.broadcasted_iota(jnp.int32, shape_, dim)


def position(k):
    return jnp.where(k < 128, k, jnp.where(k < 192, k, k - 256))


def refining_matrix():
    k = np.arange(256)
    place = np.where(k < 128, k, np.where(k < 192, k, k - 256))
    n, lane = np.arange(1280) // 128, np.arange(1280) % 128
    source = n % 2 * 64 + lane // 2 + n // 2 - 2
    return jnp.asarray(place[:, None] == source[None, :], jnp.bfloat16)


def widened(x):
    n = x.shape[0]
    y = jnp.where(iota(x.shape, 2) < 64, pltpu.roll(x, 7, 1), pltpu.roll(x, 1, 1))
    return jnp.concatenate([x.reshape(n * 8, 128), y.reshape(n * 8, 128)], axis=1)


def product(x, matrix):
    high = x.astype(jnp.bfloat16)
    rest = x - high.astype(F32)
    middle = rest.astype(jnp.bfloat16)
    low = (rest - middle.astype(F32)).astype(jnp.bfloat16)
    total = jnp.dot(low, matrix, preferred_element_type=F32)
    total = total + jnp.dot(middle, matrix, preferred_element_type=F32)
    return total + jnp.dot(high, matrix, preferred_element_type=F32)


def filtered(x, band, scale):
    return product(widened(x), band).reshape(x.shape) * scale


def scale_of(width):
    return 1.0 / (2.0 * jnp.full((8, 128), width, jnp.int32).astype(F32) + 1.0)


def if_inside(place_ref, x):
    return jnp.where(jnp.full((8, 128), place_ref[1], jnp.int32) > 0, x, 0.0)


def if_odd(place_ref, odd, even):
    return jnp.where(jnp.full((8, 128), place_ref[0], jnp.int32) > 0, odd, even)


def filter_kernel(
    place_ref, widths_hbm, v_hbm, w0_ref, w1_ref, old_ref, band_ref, widths_ref, v_ref, sems
):
    fetch = [pltpu.make_async_copy(widths_hbm, widths_ref, sems.at[0])]
    for b in range(2):
        at = pl.ds(b * 16, 16)
        fetch.append(pltpu.make_async_copy(v_hbm.at[at], v_ref.at[at], sems.at[1 + b]))
    for copy in fetch:
        copy.start()
    away = jnp.abs(position(iota((256, 128), 0)) - iota((256, 128), 1))
    fetch[0].wait()
    scales = []
    for r in range(2):
        width = widths_ref[r + place_ref[0] * (1 - 2 * r)]
        inside = away <= jnp.full((256, 128), width, jnp.int32)
        band_ref[r] = jnp.where(inside, 1.0, 0.0).astype(jnp.bfloat16)
        scales.append(scale_of(width))
    for b in range(2):
        at = pl.ds(b * 16, 16)
        fetch[1 + b].wait()
        top, bottom = (v_ref[at, pl.ds(n, 8, stride=2), :] for n in range(2))
        for r, out in ((0, w0_ref), (1, w1_ref)):
            x = if_odd(place_ref, top, bottom) if r else if_odd(place_ref, bottom, top)
            old_ref[r, at] = x
            out[at] = filtered(x, band_ref[r], scales[r])


def split_kernel(place_ref, e_hbm, far_ref, far_late_ref, near_ref, e_ref, sems):
    fetch = []
    for part in range(4):
        at = pl.ds(part * 32, 32)
        fetch.append(pltpu.make_async_copy(e_hbm.at[at], e_ref.at[at], sems.at[part]))
        fetch[-1].start()
    for part in range(4):
        fetch[part].wait()
        out = far_late_ref if part else far_ref
        first = max(part - 1, 0) * 32

        def body(b, carry, part=part, out=out, first=first):
            at = pl.ds(part * 32 + b * 8, 8)
            top, bottom = (e_ref[at, pl.ds(n, 8, stride=2), :] for n in range(2))
            out[pl.ds(first + b * 8, 8)] = if_odd(place_ref, bottom, top)
            near_ref[at] = if_odd(place_ref, top, bottom)
            return carry

        lax.fori_loop(0, 4, body, 0)


def planes_kernel(place_ref, src_ref, wgt_ref, msk_ref, inn_ref, planes_ref, mask_ref, target_ref):
    parent = iota((8, 128), 0) * 128 + iota((8, 128), 1) // 2
    odd = jnp.full((8, 128), place_ref[0], jnp.int32)
    for j in range(8):
        half, fr = j // 4, j % 4
        at, mirrored = pl.ds(j, 8, stride=8), pl.ds(half * 4 + 3 - fr, 8, stride=8)

        def row(ref, n, at=at, mirrored=mirrored):
            return jnp.where(odd > 0, ref[n, mirrored, :], ref[n, at, :])

        own_row = jnp.where(odd > 0, 1 - fr // 2, fr // 2)
        codes, weights = [], []
        for s in range(4):
            src = row(src_ref, s)
            row_shift = lax.shift_right_logical(src, 10) - (own_row + 1)
            row_shift = jnp.where(odd > 0, -row_shift, row_shift)
            col = jnp.bitwise_and(src, 1023)
            col_shift = jnp.bitwise_and(col - parent - half * 64 + 2, 1023) - 2
            codes.append((row_shift + 1) * 5 + col_shift + 2)
            weights.append(row(wgt_ref, s))
        for n in range(15):
            total = jnp.where(codes[0] == n, weights[0], 0.0)
            for s in range(1, 4):
                total = total + jnp.where(codes[s] == n, weights[s], 0.0)
            planes_ref[n, j] = total
        for t in range(4):
            mask_ref[t, j] = row(msk_ref, t).astype(F32)
            target_ref[t, j] = row(inn_ref, t)


def members(e_refs, q, piece):
    if q < 2:
        return e_refs[q * 2 + piece], 0
    return e_refs[q + 2], PIECES[piece][0] * 4


def first_kernel(place_ref, w0_ref, w1_ref, far_ref, near_ref, *refs):
    *e_refs, part_ref = refs
    sums = (jnp.zeros((8, 128), F32),) * 8
    for piece, (first, count) in enumerate(PIECES):

        def body(n, sums, piece=piece, first=first):
            m = first + n
            a, b = w0_ref[m], w1_ref[m]
            f0 = C_MID * a + C_SIDE * (if_inside(place_ref, far_ref[m]) + b)
            f1 = C_MID * b + C_SIDE * (a + near_ref[m])
            sums = list(sums)
            for t in range(4):
                sums[t] = sums[t] + e_refs[piece][n * 4 + t] * f0
                sums[4 + t] = sums[4 + t] + e_refs[2][m * 4 + t] * f1
            return tuple(sums)

        sums = lax.fori_loop(0, count, body, sums, unroll=8)
    for n in range(8):
        part_ref[n] = sums[n]


def sum_kernel(parts_ref, a_ref, b_ref):
    count = a_ref.shape[0]
    for n in range(2 * count):
        total = (parts_ref[0, n] + parts_ref[1, n]) + (parts_ref[2, n] + parts_ref[3, n])
        if n < count:
            a_ref[n] = total
        else:
            b_ref[n - count] = total


def stencil(a, b):
    lane = iota((8, 128), 1)
    a1, b1 = pltpu.roll(a, 1, 1), pltpu.roll(b, 1, 1)
    left_a = jnp.where(lane == 0, pltpu.roll(b1, 1, 0), a1)
    left_b = jnp.where(lane == 0, a1, b1)
    a2, b2 = pltpu.roll(a, 127, 1), pltpu.roll(b, 127, 1)
    right_a = jnp.where(lane == 127, b2, a2)
    right_b = jnp.where(lane == 127, pltpu.roll(a2, 7, 0), b2)
    return 0.5 * a + 0.25 * (left_a + right_a), 0.5 * b + 0.25 * (left_b + right_b)


def observe(rows, planes_ref, mask_ref, target_ref, refine_ref, gather_ref, u_ref, far_ref, near_ref):
    window = jnp.stack([rows[t][q] for t in range(4) for q in range(4)])
    u_ref[...] = product(widened(window), refine_ref[...])

    def piece(t, q, d, half):
        n = d * 2 + half
        return u_ref[pl.ds((t * 4 + q) * 8, 8), pl.ds(n * 128, 128)]

    back = {}
    for r in range(2):
        fine = {}
        for half in range(2):
            for rs in range(-1, 2):
                for d in range(5):
                    u = [piece(t, r + 1 + rs, d, half) for t in range(4)]
                    for fr in (2 * r, 2 * r + 1):
                        plane = planes_ref[(rs + 1) * 5 + d, half * 4 + fr]
                        for t in range(4):
                            key = (t, fr, half)
                            fine[key] = fine[key] + plane * u[t] if key in fine else plane * u[t]
        for t in range(4):
            for fr in (2 * r, 2 * r + 1):
                pair = stencil(fine[t, fr, 0], fine[t, fr, 1])
                pair = [
                    mask_ref[t, half * 4 + fr] * (pair[half] - target_ref[t, half * 4 + fr])
                    for half in range(2)
                ]
                back[t, fr, 0], back[t, fr, 1] = stencil(*pair)
    for half in range(2):
        for d in range(5):
            n = d * 2 + half
            for q in range(4):
                z = [None] * 4
                for fr in range(4):
                    rs = q - 1 - fr // 2
                    if -1 <= rs <= 1:
                        plane = planes_ref[(rs + 1) * 5 + d, half * 4 + fr]
                        for t in range(4):
                            term = plane * back[t, fr, half]
                            z[t] = term if z[t] is None else z[t] + term
                for t in range(4):
                    u_ref[pl.ds((t * 4 + q) * 8, 8), pl.ds(n * 128, 128)] = z[t]
    total = None
    for d in range(5):
        term = product(u_ref[:, d * 256 : d * 256 + 256], gather_ref[d * 256 : d * 256 + 256, :])
        total = term if total is None else total + term
    own, beside = total[:, :128].reshape(16, 8, 128), total[:, 128:].reshape(16, 8, 128)
    head = iota((16, 8, 128), 2) < 64
    landed = own + jnp.where(head, pltpu.roll(beside, 1, 1), pltpu.roll(beside, 7, 1))
    for t in range(4):
        far_ref[t], far_ref[4 + t] = landed[t * 4], landed[t * 4 + 1]
        near_ref[t], near_ref[4 + t] = landed[t * 4 + 3], landed[t * 4 + 2]


def first_observe_kernel(far_ref, c0_ref, c1_ref, near_ref, *refs):
    observe([[ref[t] for ref in (far_ref, c0_ref, c1_ref, near_ref)] for t in range(4)], *order(refs))


def second_observe_kernel(*refs):
    rows = joined(*refs[:4])
    observe([[rows[q][t] for q in range(4)] for t in range(4)], *order(refs[4:]))


def order(refs):
    *fields, far_ref, near_ref, u_ref = refs
    return *fields, u_ref, far_ref, near_ref


def joined(far_ref, near_ref, from_far_ref, from_near_ref):
    rows = [None] * 4
    for mine, theirs, halo, own in ((far_ref, from_far_ref, 0, 1), (near_ref, from_near_ref, 3, 2)):
        rows[halo] = [mine[t] + theirs[4 + t] for t in range(4)]
        rows[own] = [mine[4 + t] + theirs[t] for t in range(4)]
    return rows


def adjoint_rows(place_ref, refs):
    rows = joined(*refs)
    rows[0] = [if_inside(place_ref, x) for x in rows[0]]
    return rows


def smoothed_back(e_refs, rows, s_ref):
    for piece, (first, count) in enumerate(PIECES):

        def body(b, carry, piece=piece, first=first):
            back = []
            for q in range(4):
                ref, start = members(e_refs, q, piece)
                x = ref[pl.ds(start + b * 16, 16)].reshape(4, 4, 8, 128)
                total = x[:, 0] * rows[q][0]
                for t in range(1, 4):
                    total = total + x[:, t] * rows[q][t]
                back.append(total)
            at = pl.ds(first + b * 4, 4)
            for r in range(2):
                s_ref[r, at] = C_MID * back[r + 1] + C_SIDE * (back[r] + back[r + 2])
            return carry

        lax.fori_loop(0, count // 4, body, 0, unroll=2)


def middle_kernel(place_ref, lf_ref, ln_ref, rf_ref, rn_ref, *refs):
    *e_refs, band_ref, v_ref, new_ref, part_ref, s_ref, w_ref = refs
    rows = adjoint_rows(place_ref, (lf_ref, ln_ref, rf_ref, rn_ref))
    smoothed_back(e_refs, rows, s_ref)
    chunks = [(r, pl.ds(b * 16, 16)) for b in range(2) for r in range(2)]
    scales = [scale_of(place_ref[2 + r]) for r in range(2)]
    fresh = []
    for r, at in chunks:
        old = v_ref[r, at]
        gradient = old + filtered(s_ref[r, at], band_ref[r], scales[r])
        fresh.append(old - STEP_SIZE * gradient)
        new_ref[r, at] = fresh[-1]
    for (r, at), new in zip(chunks, fresh):
        w_ref[r, at] = filtered(new, band_ref[r], scales[r])
    sums = (jnp.zeros((8, 128), F32),) * 16
    for piece, (first, count) in enumerate(PIECES):

        def body(b, sums, piece=piece, first=first):
            sums = list(sums)
            for i in range(4):
                n = b * 4 + i
                w = [w_ref[r, first + n] for r in range(2)]
                forward = [
                    C_SIDE * w[0],
                    C_MID * w[0] + C_SIDE * w[1],
                    C_MID * w[1] + C_SIDE * w[0],
                    C_SIDE * w[1],
                ]
                for q in range(4):
                    ref, start = members(e_refs, q, piece)
                    for t in range(4):
                        x = ref[start + n * 4 + t]
                        sums[q * 4 + t] = sums[q * 4 + t] + x * forward[q]
            return tuple(sums)

        sums = lax.fori_loop(0, count // 4, body, sums, unroll=2)
    for t in range(4):
        part_ref[t], part_ref[4 + t] = if_inside(place_ref, sums[t]), sums[4 + t]
        part_ref[8 + t], part_ref[12 + t] = sums[12 + t], sums[8 + t]


def last_kernel(place_ref, lf_ref, ln_ref, rf_ref, rn_ref, *refs):
    *e_refs, band_ref, v_ref, out_ref, s_ref = refs
    rows = adjoint_rows(place_ref, (lf_ref, ln_ref, rf_ref, rn_ref))
    smoothed_back(e_refs, rows, s_ref)
    scales = [scale_of(place_ref[2 + r]) for r in range(2)]
    for b in range(2):
        at = pl.ds(b * 16, 16)
        new = []
        for r in range(2):
            old = v_ref[r, at]
            gradient = old + filtered(s_ref[r, at], band_ref[r], scales[r])
            new.append(old - STEP_SIZE * gradient)
        out_ref[at, pl.ds(0, 8, stride=2), :] = if_odd(place_ref, new[1], new[0])
        out_ref[at, pl.ds(1, 8, stride=2), :] = if_odd(place_ref, new[0], new[1])


def from_far(x):
    bands = lax.axis_size("lat")
    pairs = [(i, i if i in (0, bands - 1) else i + (1 if i % 2 else -1)) for i in range(bands)]
    return lax.ppermute(x, "lat", pairs)


def from_near(x):
    return lax.ppermute(x, "lat", [(i, i ^ 1) for i in range(lax.axis_size("lat"))])


def swapped(far, near):
    return from_far(far), from_near(near)


def tiles(x):
    (rows, cols) = x.shape[-2:]
    x = x.reshape(-1, rows, cols // 128, 128).transpose(0, 2, 1, 3)
    return x.reshape(-1, cols // 128 * rows, 128)


def descent(control, ensemble, widths, interp_source, interp_weight, obs_mask, innovation):
    v = tiles(control)
    e = tiles(ensemble)
    lat, last = lax.axis_index("lat"), lax.axis_size("lat") - 1
    odd = lat % 2
    ends = jnp.stack([odd, (lat != 0) & (lat != last)]).astype(jnp.int32)
    place = jnp.concatenate([ends, jnp.where(odd > 0, widths[::-1], widths)])
    scalars = (place,)
    row, rows = shape(32, 8, 128), shape(2, 32, 8, 128)
    band = jax.ShapeDtypeStruct((2, 256, 128), jnp.bfloat16)
    w0, w1, old, band = call(
        filter_kernel,
        (row, row, rows, band),
        (),
        (ends,),
        (
            pltpu.SMEM((2,), jnp.int32),
            pltpu.VMEM((32, 16, 128), F32),
            pltpu.SemaphoreType.DMA((3,)),
        ),
        (widths, v),
    )
    far, near = swapped(w0, w1)
    e0, e0_late, e1 = call(
        split_kernel,
        (shape(32, 8, 128), shape(96, 8, 128), shape(128, 8, 128)),
        (),
        scalars,
        (pltpu.VMEM((128, 16, 128), F32), pltpu.SemaphoreType.DMA((4,))),
        (e,),
    )
    ensembles = (*(from_far(e0), from_far(e0_late)), *(e0, e0_late, e1, from_near(e1)), band)
    fields = call(
        planes_kernel,
        (shape(15, 8, 8, 128), shape(4, 8, 8, 128), shape(4, 8, 8, 128)),
        tuple(tiles(x) for x in (interp_source, interp_weight, obs_mask, innovation)),
        scalars,
    )
    refine = refining_matrix()
    fields = tuple(fields) + (refine, refine.T)
    part = call(
        first_kernel, shape(8, 8, 128), (w0, w1, far, near, e0, e0_late, e1), scalars
    )
    four, eight = shape(4, 8, 128), shape(8, 8, 128)
    c0, c1 = call(sum_kernel, (four, four), (lax.all_gather(part, "mem"),))
    far, near = swapped(c0, c1)
    refined = (pltpu.VMEM((128, 1280), F32),)
    sent = call(
        first_observe_kernel, (eight, eight), (far, c0, c1, near) + fields, scratch=refined
    )
    smoothed = (pltpu.VMEM((2, 32, 8, 128), F32),)
    new, part = call(
        middle_kernel,
        (rows, shape(16, 8, 128)),
        tuple(sent) + swapped(*sent) + ensembles + (old,),
        scalars,
        smoothed * 2,
    )
    sent = call(sum_kernel, (eight, eight), (lax.all_gather(part, "mem"),))
    sent = call(
        second_observe_kernel,
        (eight, eight),
        tuple(sent) + swapped(*sent) + fields,
        scratch=refined,
    )
    out = call(
        last_kernel,
        shape(32, 16, 128),
        tuple(sent) + swapped(*sent) + ensembles + (new,),
        scalars,
        smoothed,
    )
    return out.reshape(32, 8, 2, 128).transpose(0, 2, 1, 3).reshape(control.shape)


def solution(mesh):
    in_specs = (
        P("mem", "lat", None),
        P("mem", None, "lat", None),
        P("lat"),
        P(None, "lat", None),
        P(None, "lat", None),
        P(None, "lat", None),
        P(None, "lat", None),
    )
    out_specs = P("mem", "lat", None)
    return jax.shard_map(descent, mesh=mesh, in_specs=in_specs, out_specs=out_specs, check_vma=False)
```

```python
import jax
import jax.numpy as jnp
import numpy as np
from jax import lax
from jax.experimental import pallas as pl
from jax.experimental.pallas import tpu as pltpu
from jax.sharding import PartitionSpec as P

STEP_SIZE = 0.5
C_MID = 0.5
C_SIDE = 0.25

F32 = jnp.float32
LIMIT = 40 * 1024 * 1024
PIECES = ((0, 8), (8, 24))


def shape(*dims):
    return jax.ShapeDtypeStruct(dims, F32)


def call(kernel, outs, args, scalars=(), scratch=(), far_args=(), out_space=pltpu.VMEM):
    in_specs = [pl.BlockSpec(memory_space=pltpu.SMEM)] * len(scalars)
    in_specs += [pl.BlockSpec(memory_space=pltpu.HBM)] * len(far_args)
    in_specs += [pl.BlockSpec(memory_space=pltpu.VMEM)] * len(args)
    far_args = tuple(pltpu.with_memory_space_constraint(x, pltpu.HBM) for x in far_args)
    args = tuple(scalars) + far_args + tuple(args)
    return pl.pallas_call(
        kernel,
        out_shape=outs,
        in_specs=in_specs,
        out_specs=jax.tree.map(lambda _: pl.BlockSpec(memory_space=out_space), outs),
        scratch_shapes=list(scratch),
        compiler_params=pltpu.CompilerParams(vmem_limit_bytes=LIMIT),
        cost_estimate=pl.CostEstimate(flops=1_000_000, transcendentals=0, bytes_accessed=1_000_000),
    )(*args)


def iota(shape_, dim):
    return lax.broadcasted_iota(jnp.int32, shape_, dim)


def position(k):
    return jnp.where(k < 128, k, jnp.where(k < 192, k, k - 256))


def refining_matrix():
    k = np.arange(256)
    place = np.where(k < 128, k, np.where(k < 192, k, k - 256))
    n, lane = np.arange(1280) // 128, np.arange(1280) % 128
    source = n % 2 * 64 + lane // 2 + n // 2 - 2
    return jnp.asarray(place[:, None] == source[None, :], jnp.bfloat16)


def widened(x):
    n = x.shape[0]
    y = jnp.where(iota(x.shape, 2) < 64, pltpu.roll(x, 7, 1), pltpu.roll(x, 1, 1))
    return jnp.concatenate([x.reshape(n * 8, 128), y.reshape(n * 8, 128)], axis=1)


def product(x, matrix):
    high = x.astype(jnp.bfloat16)
    rest = x - high.astype(F32)
    middle = rest.astype(jnp.bfloat16)
    low = (rest - middle.astype(F32)).astype(jnp.bfloat16)
    total = jnp.dot(low, matrix, preferred_element_type=F32)
    total = total + jnp.dot(middle, matrix, preferred_element_type=F32)
    return total + jnp.dot(high, matrix, preferred_element_type=F32)


def filtered(x, band, scale):
    return product(widened(x), band).reshape(x.shape) * scale


def scale_of(width):
    return 1.0 / (2.0 * jnp.full((8, 128), width, jnp.int32).astype(F32) + 1.0)


def if_inside(place_ref, x):
    return jnp.where(jnp.full((8, 128), place_ref[1], jnp.int32) > 0, x, 0.0)


def if_odd(place_ref, odd, even):
    return jnp.where(jnp.full((8, 128), place_ref[0], jnp.int32) > 0, odd, even)


def opening_kernel(
    place_ref, widths_hbm, v_hbm, e_hbm,
    w0_ref, w1_ref, old_ref, band_ref, scale_ref, far_ref, far_late_ref, near_ref,
    widths_ref, v_ref, e_ref, sems,
):
    fetch = [pltpu.make_async_copy(widths_hbm, widths_ref, sems.at[0])]
    for b in range(2):
        at = pl.ds(b * 16, 16)
        fetch.append(pltpu.make_async_copy(v_hbm.at[at], v_ref.at[at], sems.at[1 + b]))
    for part in range(4):
        at = pl.ds(part * 32, 32)
        fetch.append(pltpu.make_async_copy(e_hbm.at[at], e_ref.at[at], sems.at[3 + part]))
    for copy in fetch:
        copy.start()
    away = jnp.abs(position(iota((256, 128), 0)) - iota((256, 128), 1))
    fetch[0].wait()
    scales = []
    for r in range(2):
        width = widths_ref[r + place_ref[0] * (1 - 2 * r)]
        inside = away <= jnp.full((256, 128), width, jnp.int32)
        band_ref[r] = jnp.where(inside, 1.0, 0.0).astype(jnp.bfloat16)
        scales.append(scale_of(width))
        scale_ref[r] = scales[r]
    for b in range(2):
        at = pl.ds(b * 16, 16)
        fetch[1 + b].wait()
        top, bottom = (v_ref[at, pl.ds(n, 8, stride=2), :] for n in range(2))
        for r, out in ((0, w0_ref), (1, w1_ref)):
            x = if_odd(place_ref, top, bottom) if r else if_odd(place_ref, bottom, top)
            old_ref[r, at] = x
            out[at] = filtered(x, band_ref[r], scales[r])
    for part in range(4):
        fetch[3 + part].wait()
        out = far_late_ref if part else far_ref
        first = max(part - 1, 0) * 32

        def body(b, carry, part=part, out=out, first=first):
            at = pl.ds(part * 32 + b * 16, 16)
            top, bottom = (e_ref[at, pl.ds(n, 8, stride=2), :] for n in range(2))
            out[pl.ds(first + b * 16, 16)] = if_odd(place_ref, bottom, top)
            near_ref[at] = if_odd(place_ref, top, bottom)
            return carry

        lax.fori_loop(0, 2, body, 0)


def planes_kernel(place_ref, src_ref, wgt_ref, msk_ref, inn_ref, planes_ref, mask_ref, target_ref):
    parent = iota((8, 128), 0) * 128 + iota((8, 128), 1) // 2
    odd = jnp.full((8, 128), place_ref[0], jnp.int32)
    for j in range(8):
        half, fr = j // 4, j % 4
        at = pl.ds(j + place_ref[0] * (3 - 2 * fr), 8, stride=8)

        def row(ref, n, at=at):
            return ref[n, at, :]

        own_row = jnp.where(odd > 0, 1 - fr // 2, fr // 2)
        codes, weights = [], []
        for s in range(4):
            src = row(src_ref, s)
            row_shift = lax.shift_right_logical(src, 10) - (own_row + 1)
            row_shift = jnp.where(odd > 0, -row_shift, row_shift)
            col = jnp.bitwise_and(src, 1023)
            col_shift = jnp.bitwise_and(col - parent - half * 64 + 2, 1023) - 2
            codes.append((row_shift + 1) * 5 + col_shift + 2)
            weights.append(row(wgt_ref, s))
        for n in range(15):
            total = jnp.where(codes[0] == n, weights[0], 0.0)
            for s in range(1, 4):
                total = total + jnp.where(codes[s] == n, weights[s], 0.0)
            planes_ref[n, j] = total
        for t in range(4):
            mask_ref[t, j] = row(msk_ref, t).astype(F32)
            target_ref[t, j] = row(inn_ref, t)


def members(e_refs, q, piece):
    if q < 2:
        return e_refs[q * 2 + piece], 0
    return e_refs[q + 2], PIECES[piece][0] * 4


def first_kernel(place_ref, w0_ref, w1_ref, far_ref, near_ref, *refs):
    *e_refs, part_ref = refs
    sums = (jnp.zeros((8, 128), F32),) * 8
    for piece, (first, count) in enumerate(PIECES):

        def body(n, sums, piece=piece, first=first):
            m = first + n
            a, b = w0_ref[m], w1_ref[m]
            f0 = C_MID * a + C_SIDE * (if_inside(place_ref, far_ref[m]) + b)
            f1 = C_MID * b + C_SIDE * (a + near_ref[m])
            sums = list(sums)
            for t in range(4):
                sums[t] = sums[t] + e_refs[piece][n * 4 + t] * f0
                sums[4 + t] = sums[4 + t] + e_refs[2][m * 4 + t] * f1
            return tuple(sums)

        sums = lax.fori_loop(0, count, body, sums, unroll=8)
    for n in range(8):
        part_ref[n] = sums[n]


def sum_kernel(parts_ref, a_ref, b_ref):
    count = a_ref.shape[0]
    for n in range(2 * count):
        total = (parts_ref[0, n] + parts_ref[1, n]) + (parts_ref[2, n] + parts_ref[3, n])
        if n < count:
            a_ref[n] = total
        else:
            b_ref[n - count] = total


def stencil(a, b):
    lane = iota((8, 128), 1)
    a1, b1 = pltpu.roll(a, 1, 1), pltpu.roll(b, 1, 1)
    left_a = jnp.where(lane == 0, pltpu.roll(b1, 1, 0), a1)
    left_b = jnp.where(lane == 0, a1, b1)
    a2, b2 = pltpu.roll(a, 127, 1), pltpu.roll(b, 127, 1)
    right_a = jnp.where(lane == 127, b2, a2)
    right_b = jnp.where(lane == 127, pltpu.roll(a2, 7, 0), b2)
    return 0.5 * a + 0.25 * (left_a + right_a), 0.5 * b + 0.25 * (left_b + right_b)


def observe(rows, planes_ref, mask_ref, target_ref, refine_ref, gather_ref, u_ref, far_ref, near_ref):
    window = jnp.stack([rows[t][q] for t in range(4) for q in range(4)])
    u_ref[...] = product(widened(window), refine_ref[...])

    def piece(t, q, d, half):
        n = d * 2 + half
        return u_ref[pl.ds((t * 4 + q) * 8, 8), pl.ds(n * 128, 128)]

    back = {}
    for r in range(2):
        fine = {}
        for half in range(2):
            for rs in range(-1, 2):
                for d in range(5):
                    u = [piece(t, r + 1 + rs, d, half) for t in range(4)]
                    for fr in (2 * r, 2 * r + 1):
                        plane = planes_ref[(rs + 1) * 5 + d, half * 4 + fr]
                        for t in range(4):
                            key = (t, fr, half)
                            fine[key] = fine[key] + plane * u[t] if key in fine else plane * u[t]
        for t in range(4):
            for fr in (2 * r, 2 * r + 1):
                pair = stencil(fine[t, fr, 0], fine[t, fr, 1])
                pair = [
                    mask_ref[t, half * 4 + fr] * (pair[half] - target_ref[t, half * 4 + fr])
                    for half in range(2)
                ]
                back[t, fr, 0], back[t, fr, 1] = stencil(*pair)
    for half in range(2):
        for d in range(5):
            n = d * 2 + half
            for q in range(4):
                z = [None] * 4
                for fr in range(4):
                    rs = q - 1 - fr // 2
                    if -1 <= rs <= 1:
                        plane = planes_ref[(rs + 1) * 5 + d, half * 4 + fr]
                        for t in range(4):
                            term = plane * back[t, fr, half]
                            z[t] = term if z[t] is None else z[t] + term
                for t in range(4):
                    u_ref[pl.ds((t * 4 + q) * 8, 8), pl.ds(n * 128, 128)] = z[t]
    total = None
    for d in range(5):
        term = product(u_ref[:, d * 256 : d * 256 + 256], gather_ref[d * 256 : d * 256 + 256, :])
        total = term if total is None else total + term
    own, beside = total[:, :128].reshape(16, 8, 128), total[:, 128:].reshape(16, 8, 128)
    head = iota((16, 8, 128), 2) < 64
    landed = own + jnp.where(head, pltpu.roll(beside, 1, 1), pltpu.roll(beside, 7, 1))
    for t in range(4):
        far_ref[t], far_ref[4 + t] = landed[t * 4], landed[t * 4 + 1]
        near_ref[t], near_ref[4 + t] = landed[t * 4 + 3], landed[t * 4 + 2]


def first_observe_kernel(far_ref, c0_ref, c1_ref, near_ref, *refs):
    observe([[ref[t] for ref in (far_ref, c0_ref, c1_ref, near_ref)] for t in range(4)], *order(refs))


def second_observe_kernel(*refs):
    rows = joined(*refs[:4])
    observe([[rows[q][t] for q in range(4)] for t in range(4)], *order(refs[4:]))


def order(refs):
    *fields, far_ref, near_ref, u_ref = refs
    return *fields, u_ref, far_ref, near_ref


def joined(far_ref, near_ref, from_far_ref, from_near_ref):
    rows = [None] * 4
    for mine, theirs, halo, own in ((far_ref, from_far_ref, 0, 1), (near_ref, from_near_ref, 3, 2)):
        rows[halo] = [mine[t] + theirs[4 + t] for t in range(4)]
        rows[own] = [mine[4 + t] + theirs[t] for t in range(4)]
    return rows


def adjoint_rows(place_ref, refs):
    rows = joined(*refs)
    rows[0] = [if_inside(place_ref, x) for x in rows[0]]
    return rows


def smoothed_back(e_refs, rows, s_ref):
    for piece, (first, count) in enumerate(PIECES):

        def body(b, carry, piece=piece, first=first):
            back = []
            for q in range(4):
                ref, start = members(e_refs, q, piece)
                x = ref[pl.ds(start + b * 16, 16)].reshape(4, 4, 8, 128)
                total = x[:, 0] * rows[q][0]
                for t in range(1, 4):
                    total = total + x[:, t] * rows[q][t]
                back.append(total)
            at = pl.ds(first + b * 4, 4)
            for r in range(2):
                s_ref[r, at] = C_MID * back[r + 1] + C_SIDE * (back[r] + back[r + 2])
            return carry

        lax.fori_loop(0, count // 4, body, 0, unroll=2)


def middle_kernel(place_ref, lf_ref, ln_ref, rf_ref, rn_ref, *refs):
    *e_refs, band_ref, scale_ref, v_ref, new_ref, part_ref, s_ref, w_ref = refs
    rows = adjoint_rows(place_ref, (lf_ref, ln_ref, rf_ref, rn_ref))
    smoothed_back(e_refs, rows, s_ref)
    chunks = [(r, pl.ds(b * 16, 16)) for b in range(2) for r in range(2)]
    scales = [scale_ref[r] for r in range(2)]
    fresh = []
    for r, at in chunks:
        old = v_ref[r, at]
        gradient = old + filtered(s_ref[r, at], band_ref[r], scales[r])
        fresh.append(old - STEP_SIZE * gradient)
        new_ref[r, at] = fresh[-1]
    for (r, at), new in zip(chunks, fresh):
        w_ref[r, at] = filtered(new, band_ref[r], scales[r])
    sums = (jnp.zeros((8, 128), F32),) * 16
    for piece, (first, count) in enumerate(PIECES):

        def body(b, sums, piece=piece, first=first):
            sums = list(sums)
            for i in range(4):
                n = b * 4 + i
                w = [w_ref[r, first + n] for r in range(2)]
                forward = [
                    C_SIDE * w[0],
                    C_MID * w[0] + C_SIDE * w[1],
                    C_MID * w[1] + C_SIDE * w[0],
                    C_SIDE * w[1],
                ]
                for q in range(4):
                    ref, start = members(e_refs, q, piece)
                    for t in range(4):
                        x = ref[start + n * 4 + t]
                        sums[q * 4 + t] = sums[q * 4 + t] + x * forward[q]
            return tuple(sums)

        sums = lax.fori_loop(0, count // 4, body, sums, unroll=2)
    for t in range(4):
        part_ref[t], part_ref[4 + t] = if_inside(place_ref, sums[t]), sums[4 + t]
        part_ref[8 + t], part_ref[12 + t] = sums[12 + t], sums[8 + t]


def last_kernel(place_ref, lf_ref, ln_ref, rf_ref, rn_ref, *refs):
    *e_refs, band_ref, scale_ref, v_ref, out_hbm, s_ref, out_ref, sems = refs
    rows = adjoint_rows(place_ref, (lf_ref, ln_ref, rf_ref, rn_ref))
    smoothed_back(e_refs, rows, s_ref)
    scales = [scale_ref[r] for r in range(2)]
    store = []
    for b in range(2):
        at = pl.ds(b * 16, 16)
        new = []
        for r in range(2):
            old = v_ref[r, at]
            gradient = old + filtered(s_ref[r, at], band_ref[r], scales[r])
            new.append(old - STEP_SIZE * gradient)
        out_ref[at, pl.ds(0, 8, stride=2), :] = if_odd(place_ref, new[1], new[0])
        out_ref[at, pl.ds(1, 8, stride=2), :] = if_odd(place_ref, new[0], new[1])
        store.append(pltpu.make_async_copy(out_ref.at[at], out_hbm.at[at], sems.at[b]))
        store[b].start()
    for copy in store:
        copy.wait()


def from_far(x):
    bands = lax.axis_size("lat")
    pairs = [(i, i if i in (0, bands - 1) else i + (1 if i % 2 else -1)) for i in range(bands)]
    return lax.ppermute(x, "lat", pairs)


def from_near(x):
    return lax.ppermute(x, "lat", [(i, i ^ 1) for i in range(lax.axis_size("lat"))])


def swapped(far, near):
    return from_far(far), from_near(near)


def tiles(x):
    (rows, cols) = x.shape[-2:]
    x = x.reshape(-1, rows, cols // 128, 128).transpose(0, 2, 1, 3)
    return x.reshape(-1, cols // 128 * rows, 128)


def descent(control, ensemble, widths, interp_source, interp_weight, obs_mask, innovation):
    v = tiles(control)
    e = tiles(ensemble)
    lat, last = lax.axis_index("lat"), lax.axis_size("lat") - 1
    scalars = (jnp.stack([lat % 2, (lat != 0) & (lat != last)]).astype(jnp.int32),)
    row, rows = shape(32, 8, 128), shape(2, 32, 8, 128)
    w0, w1, old, band, scale, e0, e0_late, e1 = call(
        opening_kernel,
        (
            *(row, row, rows, jax.ShapeDtypeStruct((2, 256, 128), jnp.bfloat16)),
            *(shape(2, 8, 128), shape(32, 8, 128), shape(96, 8, 128), shape(128, 8, 128)),
        ),
        (),
        scalars,
        (
            pltpu.SMEM((2,), jnp.int32),
            pltpu.VMEM((32, 16, 128), F32),
            pltpu.VMEM((128, 16, 128), F32),
            pltpu.SemaphoreType.DMA((7,)),
        ),
        (widths, v, e),
    )
    far, near = swapped(w0, w1)
    ensembles = (
        *(from_far(e0), from_far(e0_late)), *(e0, e0_late, e1, from_near(e1)), *(band, scale)
    )
    fields = call(
        planes_kernel,
        (shape(15, 8, 8, 128), shape(4, 8, 8, 128), shape(4, 8, 8, 128)),
        tuple(tiles(x) for x in (interp_source, interp_weight, obs_mask, innovation)),
        scalars,
    )
    refine = refining_matrix()
    fields = tuple(fields) + (refine, refine.T)
    part = call(
        first_kernel, shape(8, 8, 128), (w0, w1, far, near, e0, e0_late, e1), scalars
    )
    four, eight = shape(4, 8, 128), shape(8, 8, 128)
    c0, c1 = call(sum_kernel, (four, four), (lax.all_gather(part, "mem"),))
    far, near = swapped(c0, c1)
    refined = (pltpu.VMEM((128, 1280), F32),)
    sent = call(
        first_observe_kernel, (eight, eight), (far, c0, c1, near) + fields, scratch=refined
    )
    smoothed = (pltpu.VMEM((2, 32, 8, 128), F32),)
    new, part = call(
        middle_kernel,
        (rows, shape(16, 8, 128)),
        tuple(sent) + swapped(*sent) + ensembles + (old,),
        scalars,
        smoothed * 2,
    )
    sent = call(sum_kernel, (eight, eight), (lax.all_gather(part, "mem"),))
    sent = call(
        second_observe_kernel,
        (eight, eight),
        tuple(sent) + swapped(*sent) + fields,
        scratch=refined,
    )
    out = call(
        last_kernel,
        shape(32, 16, 128),
        tuple(sent) + swapped(*sent) + ensembles + (new,),
        scalars,
        smoothed + (pltpu.VMEM((32, 16, 128), F32), pltpu.SemaphoreType.DMA((2,))),
        out_space=pltpu.HBM,
    )
    return out.reshape(32, 8, 2, 128).transpose(0, 2, 1, 3).reshape(control.shape)


def solution(mesh):
    in_specs = (
        P("mem", "lat", None),
        P("mem", None, "lat", None),
        P("lat"),
        P(None, "lat", None),
        P(None, "lat", None),
        P(None, "lat", None),
        P(None, "lat", None),
    )
    out_specs = P("mem", "lat", None)
    return jax.shard_map(descent, mesh=mesh, in_specs=in_specs, out_specs=out_specs, check_vma=False)
```

```python
import jax
import jax.numpy as jnp
import numpy as np
from jax import lax
from jax.experimental import pallas as pl
from jax.experimental.pallas import tpu as pltpu
from jax.sharding import PartitionSpec as P

STEP_SIZE = 0.5
C_MID = 0.5
C_SIDE = 0.25

F32 = jnp.float32
LIMIT = 40 * 1024 * 1024
PIECES = ((0, 8), (8, 24))


def shape(*dims):
    return jax.ShapeDtypeStruct(dims, F32)


def call(kernel, outs, args, scalars=(), scratch=(), far_args=(), out_space=pltpu.VMEM):
    in_specs = [pl.BlockSpec(memory_space=pltpu.SMEM)] * len(scalars)
    in_specs += [pl.BlockSpec(memory_space=pltpu.HBM)] * len(far_args)
    in_specs += [pl.BlockSpec(memory_space=pltpu.VMEM)] * len(args)
    far_args = tuple(pltpu.with_memory_space_constraint(x, pltpu.HBM) for x in far_args)
    args = tuple(scalars) + far_args + tuple(args)
    return pl.pallas_call(
        kernel,
        out_shape=outs,
        in_specs=in_specs,
        out_specs=jax.tree.map(lambda _: pl.BlockSpec(memory_space=out_space), outs),
        scratch_shapes=list(scratch),
        compiler_params=pltpu.CompilerParams(vmem_limit_bytes=LIMIT),
        cost_estimate=pl.CostEstimate(flops=1_000_000, transcendentals=0, bytes_accessed=1_000_000),
    )(*args)


def iota(shape_, dim):
    return lax.broadcasted_iota(jnp.int32, shape_, dim)


def position(k):
    return jnp.where(k < 128, k, jnp.where(k < 192, k, k - 256))


def refining_matrix():
    k = np.arange(256)
    place = np.where(k < 128, k, np.where(k < 192, k, k - 256))
    n, lane = np.arange(1280) // 128, np.arange(1280) % 128
    source = n % 2 * 64 + lane // 2 + n // 2 - 2
    return jnp.asarray(place[:, None] == source[None, :], jnp.bfloat16)


def widened(x):
    n = x.shape[0]
    y = jnp.where(iota(x.shape, 2) < 64, pltpu.roll(x, 7, 1), pltpu.roll(x, 1, 1))
    return jnp.concatenate([x.reshape(n * 8, 128), y.reshape(n * 8, 128)], axis=1)


def product(x, matrix):
    high = x.astype(jnp.bfloat16)
    rest = x - high.astype(F32)
    middle = rest.astype(jnp.bfloat16)
    low = (rest - middle.astype(F32)).astype(jnp.bfloat16)
    total = jnp.dot(low, matrix, preferred_element_type=F32)
    total = total + jnp.dot(middle, matrix, preferred_element_type=F32)
    return total + jnp.dot(high, matrix, preferred_element_type=F32)


def filtered(x, band, scale):
    return product(widened(x), band).reshape(x.shape) * scale


def scale_of(width):
    return 1.0 / (2.0 * jnp.full((8, 128), width, jnp.int32).astype(F32) + 1.0)


def if_inside(place_ref, x):
    return jnp.where(jnp.full((8, 128), place_ref[1], jnp.int32) > 0, x, 0.0)


def if_odd(place_ref, odd, even):
    return jnp.where(jnp.full((8, 128), place_ref[0], jnp.int32) > 0, odd, even)


def opening_kernel(
    place_ref, widths_hbm, v_hbm, e_hbm,
    w0_ref, w1_ref, old_ref, band_ref, scale_ref, far_ref, far_late_ref, near_ref,
    widths_ref, v_ref, e_ref, sems,
):
    fetch = [pltpu.make_async_copy(widths_hbm, widths_ref, sems.at[0])]
    for b in range(2):
        at = pl.ds(b * 16, 16)
        fetch.append(pltpu.make_async_copy(v_hbm.at[at], v_ref.at[at], sems.at[1 + b]))
    for part in range(4):
        at = pl.ds(part * 32, 32)
        fetch.append(pltpu.make_async_copy(e_hbm.at[at], e_ref.at[at], sems.at[3 + part]))
    for copy in fetch:
        copy.start()
    away = jnp.abs(position(iota((256, 128), 0)) - iota((256, 128), 1))
    fetch[0].wait()
    scales = []
    for r in range(2):
        width = widths_ref[r + place_ref[0] * (1 - 2 * r)]
        inside = away <= jnp.full((256, 128), width, jnp.int32)
        band_ref[r] = jnp.where(inside, 1.0, 0.0).astype(jnp.bfloat16)
        scales.append(scale_of(width))
        scale_ref[r] = scales[r]
    for b in range(2):
        at = pl.ds(b * 16, 16)
        fetch[1 + b].wait()
        top, bottom = (v_ref[at, pl.ds(n, 8, stride=2), :] for n in range(2))
        for r, out in ((0, w0_ref), (1, w1_ref)):
            x = if_odd(place_ref, top, bottom) if r else if_odd(place_ref, bottom, top)
            old_ref[r, at] = x
            out[at] = filtered(x, band_ref[r], scales[r])
    for part in range(4):
        fetch[3 + part].wait()
        out = far_late_ref if part else far_ref
        first = max(part - 1, 0) * 32

        def body(b, carry, part=part, out=out, first=first):
            at = pl.ds(part * 32 + b * 16, 16)
            top, bottom = (e_ref[at, pl.ds(n, 8, stride=2), :] for n in range(2))
            out[pl.ds(first + b * 16, 16)] = if_odd(place_ref, bottom, top)
            near_ref[at] = if_odd(place_ref, top, bottom)
            return carry

        lax.fori_loop(0, 2, body, 0)


def planes_kernel(place_ref, src_ref, wgt_ref, msk_ref, inn_ref, planes_ref, mask_ref, target_ref):
    parent = iota((8, 128), 0) * 128 + iota((8, 128), 1) // 2
    odd = jnp.full((8, 128), place_ref[0], jnp.int32)
    for j in range(8):
        half, fr = j // 4, j % 4
        at = pl.ds(j + place_ref[0] * (3 - 2 * fr), 8, stride=8)

        def row(ref, n, at=at):
            return ref[n, at, :]

        own_row = jnp.where(odd > 0, 1 - fr // 2, fr // 2)
        codes, weights = [], []
        for s in range(4):
            src = row(src_ref, s)
            row_shift = lax.shift_right_logical(src, 10) - (own_row + 1)
            row_shift = jnp.where(odd > 0, -row_shift, row_shift)
            col = jnp.bitwise_and(src, 1023)
            col_shift = jnp.bitwise_and(col - parent - half * 64 + 2, 1023) - 2
            codes.append((row_shift + 1) * 5 + col_shift + 2)
            weights.append(row(wgt_ref, s))
        for n in range(15):
            total = jnp.where(codes[0] == n, weights[0], 0.0)
            for s in range(1, 4):
                total = total + jnp.where(codes[s] == n, weights[s], 0.0)
            planes_ref[n, j] = total
        for t in range(4):
            mask_ref[t, j] = row(msk_ref, t).astype(F32)
            target_ref[t, j] = row(inn_ref, t)


def members(e_refs, q, piece):
    if q < 2:
        return e_refs[q * 2 + piece], 0
    return e_refs[q + 2], PIECES[piece][0] * 4


def first_kernel(place_ref, w0_ref, w1_ref, far_ref, near_ref, *refs):
    *e_refs, part_ref = refs
    sums = (jnp.zeros((8, 128), F32),) * 8
    for piece, (first, count) in enumerate(PIECES):

        def body(n, sums, piece=piece, first=first):
            m = first + n
            a, b = w0_ref[m], w1_ref[m]
            f0 = C_MID * a + C_SIDE * (if_inside(place_ref, far_ref[m]) + b)
            f1 = C_MID * b + C_SIDE * (a + near_ref[m])
            sums = list(sums)
            for t in range(4):
                sums[t] = sums[t] + e_refs[piece][n * 4 + t] * f0
                sums[4 + t] = sums[4 + t] + e_refs[2][m * 4 + t] * f1
            return tuple(sums)

        sums = lax.fori_loop(0, count, body, sums, unroll=8)
    for n in range(8):
        part_ref[n] = sums[n]


def sum_kernel(mine_ref, theirs_ref, a_ref, b_ref):
    count = a_ref.shape[0]
    for n in range(count):
        a_ref[n] = mine_ref[n] + theirs_ref[n]
        b_ref[n] = mine_ref[count + n] + theirs_ref[count + n]


def stencil(a, b):
    lane = iota((8, 128), 1)
    a1, b1 = pltpu.roll(a, 1, 1), pltpu.roll(b, 1, 1)
    left_a = jnp.where(lane == 0, pltpu.roll(b1, 1, 0), a1)
    left_b = jnp.where(lane == 0, a1, b1)
    a2, b2 = pltpu.roll(a, 127, 1), pltpu.roll(b, 127, 1)
    right_a = jnp.where(lane == 127, b2, a2)
    right_b = jnp.where(lane == 127, pltpu.roll(a2, 7, 0), b2)
    return 0.5 * a + 0.25 * (left_a + right_a), 0.5 * b + 0.25 * (left_b + right_b)


def observe(rows, planes_ref, mask_ref, target_ref, refine_ref, gather_ref, u_ref, far_ref, near_ref):
    window = jnp.stack([rows[t][q] for t in range(4) for q in range(4)])
    u_ref[...] = product(widened(window), refine_ref[...])

    def piece(t, q, d, half):
        n = d * 2 + half
        return u_ref[pl.ds((t * 4 + q) * 8, 8), pl.ds(n * 128, 128)]

    back = {}
    for r in range(2):
        fine = {}
        for half in range(2):
            for rs in range(-1, 2):
                for d in range(5):
                    u = [piece(t, r + 1 + rs, d, half) for t in range(4)]
                    for fr in (2 * r, 2 * r + 1):
                        plane = planes_ref[(rs + 1) * 5 + d, half * 4 + fr]
                        for t in range(4):
                            key = (t, fr, half)
                            fine[key] = fine[key] + plane * u[t] if key in fine else plane * u[t]
        for t in range(4):
            for fr in (2 * r, 2 * r + 1):
                pair = stencil(fine[t, fr, 0], fine[t, fr, 1])
                pair = [
                    mask_ref[t, half * 4 + fr] * (pair[half] - target_ref[t, half * 4 + fr])
                    for half in range(2)
                ]
                back[t, fr, 0], back[t, fr, 1] = stencil(*pair)
    for half in range(2):
        for d in range(5):
            n = d * 2 + half
            for q in range(4):
                z = [None] * 4
                for fr in range(4):
                    rs = q - 1 - fr // 2
                    if -1 <= rs <= 1:
                        plane = planes_ref[(rs + 1) * 5 + d, half * 4 + fr]
                        for t in range(4):
                            term = plane * back[t, fr, half]
                            z[t] = term if z[t] is None else z[t] + term
                for t in range(4):
                    u_ref[pl.ds((t * 4 + q) * 8, 8), pl.ds(n * 128, 128)] = z[t]
    total = None
    for d in range(5):
        term = product(u_ref[:, d * 256 : d * 256 + 256], gather_ref[d * 256 : d * 256 + 256, :])
        total = term if total is None else total + term
    own, beside = total[:, :128].reshape(16, 8, 128), total[:, 128:].reshape(16, 8, 128)
    head = iota((16, 8, 128), 2) < 64
    landed = own + jnp.where(head, pltpu.roll(beside, 1, 1), pltpu.roll(beside, 7, 1))
    for t in range(4):
        far_ref[t], far_ref[4 + t] = landed[t * 4], landed[t * 4 + 1]
        near_ref[t], near_ref[4 + t] = landed[t * 4 + 3], landed[t * 4 + 2]


def first_observe_kernel(far_ref, c0_ref, c1_ref, near_ref, *refs):
    observe([[ref[t] for ref in (far_ref, c0_ref, c1_ref, near_ref)] for t in range(4)], *order(refs))


def second_observe_kernel(*refs):
    rows = joined(*refs[:4])
    observe([[rows[q][t] for q in range(4)] for t in range(4)], *order(refs[4:]))


def order(refs):
    *fields, far_ref, near_ref, u_ref = refs
    return *fields, u_ref, far_ref, near_ref


def joined(far_ref, near_ref, from_far_ref, from_near_ref):
    rows = [None] * 4
    for mine, theirs, halo, own in ((far_ref, from_far_ref, 0, 1), (near_ref, from_near_ref, 3, 2)):
        rows[halo] = [mine[t] + theirs[4 + t] for t in range(4)]
        rows[own] = [mine[4 + t] + theirs[t] for t in range(4)]
    return rows


def adjoint_rows(place_ref, refs):
    rows = joined(*refs)
    rows[0] = [if_inside(place_ref, x) for x in rows[0]]
    return rows


def smoothed_back(e_refs, rows, s_ref):
    for piece, (first, count) in enumerate(PIECES):

        def body(b, carry, piece=piece, first=first):
            back = []
            for q in range(4):
                ref, start = members(e_refs, q, piece)
                x = ref[pl.ds(start + b * 16, 16)].reshape(4, 4, 8, 128)
                total = x[:, 0] * rows[q][0]
                for t in range(1, 4):
                    total = total + x[:, t] * rows[q][t]
                back.append(total)
            at = pl.ds(first + b * 4, 4)
            for r in range(2):
                s_ref[r, at] = C_MID * back[r + 1] + C_SIDE * (back[r] + back[r + 2])
            return carry

        lax.fori_loop(0, count // 4, body, 0, unroll=2)


def middle_kernel(place_ref, lf_ref, ln_ref, rf_ref, rn_ref, *refs):
    *e_refs, band_ref, scale_ref, v_ref, new_ref, part_ref, s_ref, w_ref = refs
    rows = adjoint_rows(place_ref, (lf_ref, ln_ref, rf_ref, rn_ref))
    smoothed_back(e_refs, rows, s_ref)
    chunks = [(r, pl.ds(b * 16, 16)) for b in range(2) for r in range(2)]
    scales = [scale_ref[r] for r in range(2)]
    fresh = []
    for r, at in chunks:
        old = v_ref[r, at]
        gradient = old + filtered(s_ref[r, at], band_ref[r], scales[r])
        fresh.append(old - STEP_SIZE * gradient)
        new_ref[r, at] = fresh[-1]
    for (r, at), new in zip(chunks, fresh):
        w_ref[r, at] = filtered(new, band_ref[r], scales[r])
    sums = (jnp.zeros((8, 128), F32),) * 16
    for piece, (first, count) in enumerate(PIECES):

        def body(b, sums, piece=piece, first=first):
            sums = list(sums)
            for i in range(4):
                n = b * 4 + i
                w = [w_ref[r, first + n] for r in range(2)]
                forward = [
                    C_SIDE * w[0],
                    C_MID * w[0] + C_SIDE * w[1],
                    C_MID * w[1] + C_SIDE * w[0],
                    C_SIDE * w[1],
                ]
                for q in range(4):
                    ref, start = members(e_refs, q, piece)
                    for t in range(4):
                        x = ref[start + n * 4 + t]
                        sums[q * 4 + t] = sums[q * 4 + t] + x * forward[q]
            return tuple(sums)

        sums = lax.fori_loop(0, count // 4, body, sums, unroll=2)
    for t in range(4):
        part_ref[t], part_ref[4 + t] = if_inside(place_ref, sums[t]), sums[4 + t]
        part_ref[8 + t], part_ref[12 + t] = sums[12 + t], sums[8 + t]


def last_kernel(place_ref, lf_ref, ln_ref, rf_ref, rn_ref, *refs):
    *e_refs, band_ref, scale_ref, v_ref, out_hbm, s_ref, out_ref, sems = refs
    rows = adjoint_rows(place_ref, (lf_ref, ln_ref, rf_ref, rn_ref))
    smoothed_back(e_refs, rows, s_ref)
    scales = [scale_ref[r] for r in range(2)]
    store = []
    for b in range(2):
        at = pl.ds(b * 16, 16)
        new = []
        for r in range(2):
            old = v_ref[r, at]
            gradient = old + filtered(s_ref[r, at], band_ref[r], scales[r])
            new.append(old - STEP_SIZE * gradient)
        out_ref[at, pl.ds(0, 8, stride=2), :] = if_odd(place_ref, new[1], new[0])
        out_ref[at, pl.ds(1, 8, stride=2), :] = if_odd(place_ref, new[0], new[1])
        store.append(pltpu.make_async_copy(out_ref.at[at], out_hbm.at[at], sems.at[b]))
        store[b].start()
    for copy in store:
        copy.wait()


def from_far(x):
    bands = lax.axis_size("lat")
    pairs = [(i, i if i in (0, bands - 1) else i + (1 if i % 2 else -1)) for i in range(bands)]
    return lax.ppermute(x, "lat", pairs)


def from_near(x):
    return lax.ppermute(x, "lat", [(i, i ^ 1) for i in range(lax.axis_size("lat"))])


def member_sum(part):
    groups = lax.axis_size("mem")
    pair = part + lax.ppermute(part, "mem", [(i, i ^ 1) for i in range(groups)])
    other = lax.ppermute(pair, "mem", [(i, (i + groups // 2) % groups) for i in range(groups)])
    half = shape(part.shape[0] // 2, 8, 128)
    return call(sum_kernel, (half, half), (pair, other))


def swapped(far, near):
    return from_far(far), from_near(near)


def tiles(x):
    (rows, cols) = x.shape[-2:]
    x = x.reshape(-1, rows, cols // 128, 128).transpose(0, 2, 1, 3)
    return x.reshape(-1, cols // 128 * rows, 128)


def descent(control, ensemble, widths, interp_source, interp_weight, obs_mask, innovation):
    v = tiles(control)
    e = tiles(ensemble)
    lat, last = lax.axis_index("lat"), lax.axis_size("lat") - 1
    scalars = (jnp.stack([lat % 2, (lat != 0) & (lat != last)]).astype(jnp.int32),)
    row, rows = shape(32, 8, 128), shape(2, 32, 8, 128)
    w0, w1, old, band, scale, e0, e0_late, e1 = call(
        opening_kernel,
        (
            *(row, row, rows, jax.ShapeDtypeStruct((2, 256, 128), jnp.bfloat16)),
            *(shape(2, 8, 128), shape(32, 8, 128), shape(96, 8, 128), shape(128, 8, 128)),
        ),
        (),
        scalars,
        (
            pltpu.SMEM((2,), jnp.int32),
            pltpu.VMEM((32, 16, 128), F32),
            pltpu.VMEM((128, 16, 128), F32),
            pltpu.SemaphoreType.DMA((7,)),
        ),
        (widths, v, e),
    )
    far, near = swapped(w0, w1)
    ensembles = (
        *(from_far(e0), from_far(e0_late)), *(e0, e0_late, e1, from_near(e1)), *(band, scale)
    )
    fields = call(
        planes_kernel,
        (shape(15, 8, 8, 128), shape(4, 8, 8, 128), shape(4, 8, 8, 128)),
        tuple(tiles(x) for x in (interp_source, interp_weight, obs_mask, innovation)),
        scalars,
    )
    refine = refining_matrix()
    fields = tuple(fields) + (refine, refine.T)
    part = call(
        first_kernel, shape(8, 8, 128), (w0, w1, far, near, e0, e0_late, e1), scalars
    )
    eight = shape(8, 8, 128)
    c0, c1 = member_sum(part)
    far, near = swapped(c0, c1)
    refined = (pltpu.VMEM((128, 1280), F32),)
    sent = call(
        first_observe_kernel, (eight, eight), (far, c0, c1, near) + fields, scratch=refined
    )
    smoothed = (pltpu.VMEM((2, 32, 8, 128), F32),)
    new, part = call(
        middle_kernel,
        (rows, shape(16, 8, 128)),
        tuple(sent) + swapped(*sent) + ensembles + (old,),
        scalars,
        smoothed * 2,
    )
    sent = member_sum(part)
    sent = call(
        second_observe_kernel,
        (eight, eight),
        tuple(sent) + swapped(*sent) + fields,
        scratch=refined,
    )
    out = call(
        last_kernel,
        shape(32, 16, 128),
        tuple(sent) + swapped(*sent) + ensembles + (new,),
        scalars,
        smoothed + (pltpu.VMEM((32, 16, 128), F32), pltpu.SemaphoreType.DMA((2,))),
        out_space=pltpu.HBM,
    )
    return out.reshape(32, 8, 2, 128).transpose(0, 2, 1, 3).reshape(control.shape)


def solution(mesh):
    in_specs = (
        P("mem", "lat", None),
        P("mem", None, "lat", None),
        P("lat"),
        P(None, "lat", None),
        P(None, "lat", None),
        P(None, "lat", None),
        P(None, "lat", None),
    )
    out_specs = P("mem", "lat", None)
    return jax.shard_map(descent, mesh=mesh, in_specs=in_specs, out_specs=out_specs, check_vma=False)
```
